8 devices in a mesh: part: 1 (over z), data: 2 (over y), time: 4 (over x, core).
Axes of the slice: x: 2, y: 2, z: 1, core: 2. Of those that a mesh axis runs over, the one named last changes fastest.
Arguments:
- x_init: float32 [4, 256, 16], P(('part', 'data'))
- w_in: bfloat16 [16, 1152], replicated
- w_out: bfloat16 [1152, 16], replicated
- mod_scale: bfloat16 [16, 1152], P('time')
- mod_shift: bfloat16 [16, 1152], P('time')
- step_size: float32 [16], P('time')
Outputs:
- output: float32 [16, 4, 256, 16], P('time', ('part', 'data'))
All inputs are finite; a program needn't handle non-finite values.
Results may differ from the reference program's by a relative error of at most 0.001.
Values are sent between devices in bfloat16 or wider.
A program may use at most 1 GiB of HBM per device.

```python
import jax
import jax.numpy as jnp
from jax import lax

TOKENS = 256
CHANNELS = 16
HIDDEN = 1152
STEPS = 16
BATCH = 4
SWEEPS = 4
HORIZON = 2


def setup_inputs(seed: int = 0, part: int = 0) -> dict:
    keys = jax.random.split(jax.random.key(seed), 8)
    x_init = jax.random.normal(jax.random.fold_in(keys[0], part), (BATCH, TOKENS, CHANNELS), jnp.float32)
    w_in = (jax.random.normal(keys[1], (CHANNELS, HIDDEN), jnp.float32) * CHANNELS ** -0.5).astype(jnp.bfloat16)
    w_out = (jax.random.normal(keys[2], (HIDDEN, CHANNELS), jnp.float32) * HIDDEN ** -0.5).astype(jnp.bfloat16)
    mod_scale = (0.5 * jax.random.normal(keys[3], (STEPS, HIDDEN), jnp.float32)).astype(jnp.bfloat16)
    mod_shift = (0.5 * jax.random.normal(keys[4], (STEPS, HIDDEN), jnp.float32)).astype(jnp.bfloat16)
    slope = jax.random.uniform(keys[5], (), jnp.float32, -3.0, 3.0)
    grid = (jnp.arange(STEPS, dtype=jnp.float32) + 0.5) / STEPS - 0.5
    weight = jnp.exp(slope * grid + 0.3 * jax.random.normal(keys[6], (STEPS,), jnp.float32))
    step_size = HORIZON * weight / jnp.sum(weight)
    return {"x_init": x_init, "w_in": w_in, "w_out": w_out, "mod_scale": mod_scale, "mod_shift": mod_shift, "step_size": step_size}


def reference(x_init, w_in, w_out, mod_scale, mod_shift, step_size):
    scale_one = 1.0 + mod_scale.astype(jnp.float32)
    shift_val = mod_shift.astype(jnp.float32)

    def drift_step(operands):
        latent, scale_row, shift_row, size_one = operands
        flat = latent.reshape(-1, latent.shape[-1]).astype(jnp.bfloat16)
        pre = jnp.dot(flat, w_in, preferred_element_type=jnp.float32)
        act = jax.nn.gelu(pre * scale_row + shift_row, approximate=True)
        out = jnp.dot(act.astype(jnp.bfloat16), w_out, preferred_element_type=jnp.float32)
        return (out * size_one).reshape(latent.shape)

    def one_sweep(latents, unused):
        drift = lax.map(drift_step, (latents, scale_one, shift_val, step_size))
        running = jnp.cumsum(drift, axis=0)
        preceding = jnp.concatenate([jnp.zeros_like(running[:1]), running[:-1]], axis=0)
        return x_init[None] + preceding, None

    start_lat = jnp.broadcast_to(x_init[None], (step_size.shape[0],) + x_init.shape)
    final, unused = lax.scan(one_sweep, start_lat, None, length=SWEEPS)
    return final
```

```python
import functools
import math

import jax
import jax.numpy as jnp
from jax import lax
from jax.experimental import pallas as pl
from jax.experimental.pallas import tpu as pltpu
from jax.sharding import PartitionSpec as P

SWEEPS = 4
LANES = 128
ROWS = 128
MESH = pl.DeviceIdType.MESH

A = 2.0 * math.sqrt(2.0 / math.pi)
B = 8.0 * math.sqrt(2.0 / math.pi) * 0.044715


def kernel(
    x_hbm, win_hbm, wout_hbm, scale_hbm, shift_hbm, step_hbm, out_ref,
    xv, win, wout, mods, steps, weights, drifts, stage,
    local_sem, mod_send, mod_recv, step_send, step_recv, out_send, out_recv,
):
    me = lax.axis_index("time")
    n_dev = 4
    per_dev = mods.shape[2]
    hidden = win.shape[1]
    partner = me + 1 - 2 * lax.rem(me, 2)
    order = [me, partner, lax.rem(me + 2, n_dev), lax.rem(partner + 2, n_dev)]
    peers = order[1:]

    barrier = pltpu.get_barrier_semaphore()
    for peer in peers:
        pl.semaphore_signal(barrier, inc=1, device_id={"time": peer}, device_id_type=MESH)

    sample = me // 2
    first = pl.multiple_of(lax.rem(me, 2) * LANES, LANES)
    loads = [
        pltpu.make_async_copy(scale_hbm, mods.at[me, 0], local_sem.at[0]),
        pltpu.make_async_copy(shift_hbm, mods.at[me, 1], local_sem.at[1]),
        pltpu.make_async_copy(step_hbm, steps.at[me], local_sem.at[2]),
        pltpu.make_async_copy(win_hbm, win, local_sem.at[3]),
        pltpu.make_async_copy(x_hbm.at[sample, :, pl.ds(first, LANES)], xv, local_sem.at[4]),
        pltpu.make_async_copy(wout_hbm, wout, local_sem.at[5]),
    ]
    for load in loads:
        load.start()
    for load in loads:
        load.wait()
    pl.semaphore_wait(barrier, len(peers))

    sends = []
    for peer in peers:
        for ref, send, recv in ((mods, mod_send, mod_recv), (steps, step_send, step_recv)):
            copy = pltpu.make_async_remote_copy(
                src_ref=ref.at[me], dst_ref=ref.at[me], send_sem=send.at[peer], recv_sem=recv.at[me],
                device_id={"time": peer}, device_id_type=MESH)
            copy.start()
            sends.append(copy)

    win_b = win[...]
    win_f = win_b.astype(jnp.float32)
    wout_b = wout[...]
    zero = jnp.zeros((16, LANES), jnp.bfloat16)
    row = lax.broadcasted_iota(jnp.int32, (16, LANES), 0)
    unit = jnp.where(row == 0, 0.5, 0.0).astype(jnp.bfloat16)

    def rhs_of(left, right):
        columns = []
        for at, value in enumerate((left, right)):
            if value is None:
                continue
            half = (value * 0.5).astype(jnp.bfloat16)
            own = [half, half, half, unit]
            blank = [zero] * 4
            columns.append(jnp.concatenate(own + blank if at == 0 else blank + own, axis=0))
        return columns[0] if len(columns) == 1 else jnp.concatenate(columns, axis=1)

    def drift_of(pair, rhs):
        total = None
        for at in range(0, hidden, ROWS):
            half = jnp.dot(weights[pair, at:at + ROWS, :], rhs, preferred_element_type=jnp.float32)
            arg = half * (half * half * B + A)
            act = half * jnp.tanh(arg) + half
            part = jnp.dot(wout_b[:, at:at + ROWS], act.astype(jnp.bfloat16), preferred_element_type=jnp.float32)
            total = part if total is None else total + part
        return total

    def prepare(group):
        for pair in range(per_dev // 2):
            rows = []
            for at in (2 * pair, 2 * pair + 1):
                scaled = win_f * mods[group, 0, at:at + 1, :].astype(jnp.float32)
                high = scaled.astype(jnp.bfloat16)
                low = (scaled - high.astype(jnp.float32)).astype(jnp.bfloat16)
                shift = jnp.broadcast_to(mods[group, 1, at:at + 1, :].astype(jnp.float32), win_f.shape)
                rows += [win_b, high, low, shift.astype(jnp.bfloat16)]
            weights[group * (per_dev // 2) + pair] = jnp.concatenate(rows, axis=0).T

    x0 = xv[...]
    rhs0 = rhs_of(x0, x0)
    for at, group in enumerate(order):
        if at > 0:
            for ref, send, recv in ((mods, mod_send, mod_recv), (steps, step_send, step_recv)):
                pltpu.make_async_remote_copy(
                    src_ref=ref.at[me], dst_ref=ref.at[group], send_sem=send.at[group], recv_sem=recv.at[group],
                    device_id={"time": group}, device_id_type=MESH).wait_recv()
        prepare(group)
        for pair in range(per_dev // 2):
            total = drift_of(group * (per_dev // 2) + pair, rhs0)
            for side in range(2):
                index = 2 * pair + side
                size = jnp.broadcast_to(steps[group][:, index:index + 1], (16, LANES))
                drifts[group * per_dev + index] = total[:, side * LANES:(side + 1) * LANES] * size

    n_steps = n_dev * per_dev
    latents = [x0]
    for index in range(n_steps - 1):
        latents.append(latents[-1] + drifts[index])

    out_copies = []
    for sweep in range(1, SWEEPS):
        last = sweep == SWEEPS - 1
        new = [x0]
        for index in range(sweep):
            new.append(latents[index + 1])
        for pair in range(n_steps // 2):
            wanted = [sweep <= index < n_steps - 1 for index in (2 * pair, 2 * pair + 1)]
            if any(wanted):
                values = [latents[2 * pair + side] if wanted[side] else None for side in range(2)]
                total = drift_of(pair, rhs_of(*values))
                column = 0
                for side in range(2):
                    if wanted[side]:
                        index = 2 * pair + side
                        size = jnp.broadcast_to(steps[index // per_dev][:, index % per_dev:index % per_dev + 1], (16, LANES))
                        new.append(new[-1] + total[:, column:column + LANES] * size)
                        column += LANES
        latents = new
    for index in range(n_steps):
        stage[index] = latents[index]
    place = (slice(None), sample, slice(None), pl.ds(first, LANES))
    for group in range(n_dev):
        copy = pltpu.make_async_remote_copy(
            src_ref=stage.at[pl.ds(group * per_dev, per_dev)], dst_ref=out_ref.at[place],
            send_sem=out_send.at[group], recv_sem=out_recv.at[me],
            device_id={"time": group}, device_id_type=MESH)

        @pl.when(me != group)
        def _():
            copy.start()

        @pl.when(me == group)
        def _():
            out_ref[place] = stage[group * per_dev:(group + 1) * per_dev]

    for copy in sends:
        copy.wait_send()
    for peer in peers:
        there = (slice(None), peer // 2, slice(None), pl.ds(pl.multiple_of(lax.rem(peer, 2) * LANES, LANES), LANES))
        done = pltpu.make_async_remote_copy(
            src_ref=stage.at[pl.ds(peer * per_dev, per_dev)], dst_ref=out_ref.at[there],
            send_sem=out_send.at[peer], recv_sem=out_recv.at[peer],
            device_id={"time": peer}, device_id_type=MESH)
        done.wait_send()
        done.wait_recv()


def solution(mesh):
    def local_run(x_init, w_in, w_out, mod_scale, mod_shift, step_size):
        samples, tokens, channels = x_init.shape
        per_dev, hidden = mod_scale.shape
        any_space = pl.BlockSpec(memory_space=pl.ANY)
        out = pl.pallas_call(
            kernel,
            out_shape=jax.ShapeDtypeStruct((per_dev, samples, channels, tokens), jnp.float32),
            in_specs=[any_space] * 6,
            out_specs=pl.BlockSpec(memory_space=pltpu.VMEM),
            scratch_shapes=[
                pltpu.VMEM((channels, LANES), jnp.float32),
                pltpu.VMEM((channels, hidden), jnp.bfloat16),
                pltpu.VMEM((channels, hidden), jnp.bfloat16),
                pltpu.VMEM((4, 2, per_dev, hidden), jnp.bfloat16),
                pltpu.VMEM((4, 1, per_dev), jnp.float32),
                pltpu.VMEM((2 * per_dev, hidden, LANES), jnp.bfloat16),
                pltpu.VMEM((4 * per_dev, channels, LANES), jnp.float32),
                pltpu.VMEM((4 * per_dev, channels, LANES), jnp.float32),
                pltpu.SemaphoreType.DMA((6,)),
                pltpu.SemaphoreType.DMA((4,)),
                pltpu.SemaphoreType.DMA((4,)),
                pltpu.SemaphoreType.DMA((4,)),
                pltpu.SemaphoreType.DMA((4,)),
                pltpu.SemaphoreType.DMA((4,)),
                pltpu.SemaphoreType.DMA((4,)),
            ],
            compiler_params=pltpu.CompilerParams(collective_id=0, has_side_effects=True),
        )(
            x_init.transpose(0, 2, 1), w_in, w_out.T, mod_scale, mod_shift,
            step_size.reshape(1, per_dev),
        )
        return out.transpose(0, 1, 3, 2)

    return jax.shard_map(
        local_run,
        mesh=mesh,
        in_specs=(P(("part", "data"), None, None), P(None, None), P(None, None), P("time", None), P("time", None), P("time")),
        out_specs=P("time", ("part", "data"), None, None),
        check_vma=False,
    )
```

```python
import functools
import math

import jax
import jax.numpy as jnp
from jax import lax
from jax.experimental import pallas as pl
from jax.experimental.pallas import tpu as pltpu
from jax.sharding import PartitionSpec as P

SWEEPS = 4
LANES = 128
ROWS = 128
AHEAD = 5
BEHIND = 1
MESH = pl.DeviceIdType.MESH

A = 2.0 * math.sqrt(2.0 / math.pi)
B = 8.0 * math.sqrt(2.0 / math.pi) * 0.044715


def kernel(
    x_hbm, win_hbm, wout_hbm, scale_hbm, shift_hbm, step_hbm, out_ref,
    xv, win, wout, mods, steps, weights, drifts, stage,
    local_sem, mod_send, mod_recv, step_send, step_recv, out_send, out_recv,
):
    me = lax.axis_index("time")
    n_dev = 4
    per_dev = mods.shape[2]
    hidden = win.shape[1]
    partner = me + 1 - 2 * lax.rem(me, 2)
    order = [me, partner, lax.rem(me + 2, n_dev), lax.rem(partner + 2, n_dev)]
    peers = order[1:]

    barrier = pltpu.get_barrier_semaphore()
    for peer in peers:
        pl.semaphore_signal(barrier, inc=1, device_id={"time": peer}, device_id_type=MESH)

    sample = me // 2
    lane = pl.multiple_of(lax.rem(me, 2) * LANES, LANES)
    loads = [
        pltpu.make_async_copy(scale_hbm, mods.at[me, 0], local_sem.at[0]),
        pltpu.make_async_copy(shift_hbm, mods.at[me, 1], local_sem.at[1]),
        pltpu.make_async_copy(step_hbm, steps.at[me], local_sem.at[2]),
        pltpu.make_async_copy(win_hbm, win, local_sem.at[3]),
        pltpu.make_async_copy(x_hbm.at[sample, :, pl.ds(lane, LANES)], xv, local_sem.at[4]),
        pltpu.make_async_copy(wout_hbm, wout, local_sem.at[5]),
    ]
    for load in loads:
        load.start()
    for load in loads:
        load.wait()
    pl.semaphore_wait(barrier, len(peers))

    sends = []
    for peer in peers:
        for ref, send, recv in ((mods, mod_send, mod_recv), (steps, step_send, step_recv)):
            copy = pltpu.make_async_remote_copy(
                src_ref=ref.at[me], dst_ref=ref.at[me], send_sem=send.at[peer], recv_sem=recv.at[me],
                device_id={"time": peer}, device_id_type=MESH)
            copy.start()
            sends.append(copy)

    win_b = win[...]
    win_f = win_b.astype(jnp.float32)
    wout_b = wout[...]
    zero = jnp.zeros((16, LANES), jnp.bfloat16)
    row = lax.broadcasted_iota(jnp.int32, (16, LANES), 0)
    unit = jnp.where(row == 0, 0.5, 0.0).astype(jnp.bfloat16)

    def rhs_of(left, right):
        columns = []
        for at, value in enumerate((left, right)):
            if value is None:
                continue
            half = (value * 0.5).astype(jnp.bfloat16)
            own = [half, half, half, unit]
            blank = [zero] * 4
            columns.append(jnp.concatenate(own + blank if at == 0 else blank + own, axis=0))
        return columns[0] if len(columns) == 1 else jnp.concatenate(columns, axis=1)

    chunks = list(range(0, hidden, ROWS))

    def run(tasks):
        todo = [(task, at) for task in tasks for at in chunks]
        halves, acts, right, total = {}, {}, {}, {}

        def first(step):
            task, at = todo[step]
            if at == 0:
                right[id(task)] = task[1]()
            halves[step] = jnp.dot(
                weights[task[0], at:at + ROWS, :], right[id(task)], preferred_element_type=jnp.float32)

        def second(step):
            task, at = todo[step]
            part = jnp.dot(wout_b[:, at:at + ROWS], acts.pop(step), preferred_element_type=jnp.float32)
            total[id(task)] = part if at == 0 else total[id(task)] + part
            if at == chunks[-1]:
                task[2](total[id(task)])

        for step in range(min(AHEAD, len(todo))):
            first(step)
        for step in range(len(todo)):
            if step + AHEAD < len(todo):
                first(step + AHEAD)
            half = halves.pop(step)
            arg = half * (half * half * B + A)
            acts[step] = (half * jnp.tanh(arg) + half).astype(jnp.bfloat16)
            if step >= BEHIND:
                second(step - BEHIND)
        for step in range(max(len(todo) - BEHIND, 0), len(todo)):
            second(step)

    def prepare(group):
        for pair in range(per_dev // 2):
            rows = []
            for at in (2 * pair, 2 * pair + 1):
                scaled = win_f * mods[group, 0, at:at + 1, :].astype(jnp.float32)
                high = scaled.astype(jnp.bfloat16)
                low = (scaled - high.astype(jnp.float32)).astype(jnp.bfloat16)
                shift = jnp.broadcast_to(mods[group, 1, at:at + 1, :].astype(jnp.float32), win_f.shape)
                rows += [win_b, high, low, shift.astype(jnp.bfloat16)]
            weights[group * (per_dev // 2) + pair] = jnp.concatenate(rows, axis=0).T

    x0 = xv[...]
    rhs0 = rhs_of(x0, x0)

    def wait_mods(group):
        for ref, send, recv in ((mods, mod_send, mod_recv), (steps, step_send, step_recv)):
            pltpu.make_async_remote_copy(
                src_ref=ref.at[me], dst_ref=ref.at[group], send_sem=send.at[group], recv_sem=recv.at[group],
                device_id={"time": group}, device_id_type=MESH).wait_recv()

    def step_of(group, index):
        return jnp.broadcast_to(steps[group][:, index:index + 1], (16, LANES))

    def opening(group, pair):
        def finish(total):
            for side in range(2):
                index = 2 * pair + side
                drifts[group * per_dev + index] = total[:, side * LANES:(side + 1) * LANES] * step_of(group, index)

        return (group * (per_dev // 2) + pair, lambda: rhs0, finish)

    pairs = range(per_dev // 2)
    prepare(order[0])
    run([opening(order[0], pair) for pair in pairs])
    wait_mods(order[1])
    prepare(order[1])
    run([opening(order[1], pair) for pair in pairs])
    for group in order[2:]:
        wait_mods(group)
    for group in order[2:]:
        prepare(group)
    run([opening(group, pair) for group in order[2:] for pair in pairs])

    n_steps = n_dev * per_dev
    latents = [x0]
    for index in range(n_steps - 1):
        latents.append(latents[-1] + drifts[index])
    history = [latents]

    def later(sweep, pair):
        wanted = [side for side in range(2) if sweep <= 2 * pair + side < n_steps - 1]

        def right():
            return rhs_of(*[history[sweep - 1][2 * pair + side] if side in wanted else None for side in range(2)])

        def finish(total):
            new = history[sweep]
            for at, side in enumerate(wanted):
                index = 2 * pair + side
                drift = total[:, at * LANES:(at + 1) * LANES] * step_of(index // per_dev, index % per_dev)
                new.append(new[-1] + drift)
                if sweep == SWEEPS - 1:
                    stage[index + 1] = new[-1]
                    if (index + 2) % per_dev == 0:
                        give((index + 1) // per_dev)

        return (pair, right, finish)

    place = (slice(None), sample, slice(None), pl.ds(lane, LANES))

    def give(group):
        copy = pltpu.make_async_remote_copy(
            src_ref=stage.at[pl.ds(group * per_dev, per_dev)], dst_ref=out_ref.at[place],
            send_sem=out_send.at[group], recv_sem=out_recv.at[me],
            device_id={"time": group}, device_id_type=MESH)

        @pl.when(me != group)
        def _():
            copy.start()

        @pl.when(me == group)
        def _():
            out_ref[place] = stage[group * per_dev:(group + 1) * per_dev]

    tasks = []
    for sweep in range(1, SWEEPS):
        history.append(None)
        for pair in range(n_steps // 2):
            if 2 * pair + 1 >= sweep and 2 * pair < n_steps - 1:
                tasks.append((sweep, pair))

    def begin(sweep):
        history[sweep] = list(history[sweep - 1][:sweep + 1])
        if sweep == SWEEPS - 1:
            for index in range(sweep + 1):
                stage[index] = history[sweep][index]
                if (index + 1) % per_dev == 0:
                    give(index // per_dev)

    def task_of(sweep, pair):
        task = later(sweep, pair)
        if 2 * pair <= sweep <= 2 * pair + 1:
            def right():
                begin(sweep)
                return task[1]()
            return (task[0], right, task[2])
        return task

    run([task_of(sweep, pair) for sweep, pair in tasks])

    for copy in sends:
        copy.wait_send()
    for peer in peers:
        there = (slice(None), peer // 2, slice(None), pl.ds(pl.multiple_of(lax.rem(peer, 2) * LANES, LANES), LANES))
        done = pltpu.make_async_remote_copy(
            src_ref=stage.at[pl.ds(peer * per_dev, per_dev)], dst_ref=out_ref.at[there],
            send_sem=out_send.at[peer], recv_sem=out_recv.at[peer],
            device_id={"time": peer}, device_id_type=MESH)
        done.wait_send()
        done.wait_recv()


def solution(mesh):
    def local_run(x_init, w_in, w_out, mod_scale, mod_shift, step_size):
        samples, tokens, channels = x_init.shape
        per_dev, hidden = mod_scale.shape
        any_space = pl.BlockSpec(memory_space=pl.ANY)
        out = pl.pallas_call(
            kernel,
            out_shape=jax.ShapeDtypeStruct((per_dev, samples, channels, tokens), jnp.float32),
            in_specs=[any_space] * 6,
            out_specs=pl.BlockSpec(memory_space=pltpu.VMEM),
            scratch_shapes=[
                pltpu.VMEM((channels, LANES), jnp.float32),
                pltpu.VMEM((channels, hidden), jnp.bfloat16),
                pltpu.VMEM((channels, hidden), jnp.bfloat16),
                pltpu.VMEM((4, 2, per_dev, hidden), jnp.bfloat16),
                pltpu.VMEM((4, 1, per_dev), jnp.float32),
                pltpu.VMEM((2 * per_dev, hidden, LANES), jnp.bfloat16),
                pltpu.VMEM((4 * per_dev, channels, LANES), jnp.float32),
                pltpu.VMEM((4 * per_dev, channels, LANES), jnp.float32),
                pltpu.SemaphoreType.DMA((6,)),
                pltpu.SemaphoreType.DMA((4,)),
                pltpu.SemaphoreType.DMA((4,)),
                pltpu.SemaphoreType.DMA((4,)),
                pltpu.SemaphoreType.DMA((4,)),
                pltpu.SemaphoreType.DMA((4,)),
                pltpu.SemaphoreType.DMA((4,)),
            ],
            compiler_params=pltpu.CompilerParams(collective_id=0, has_side_effects=True),
        )(
            x_init.transpose(0, 2, 1), w_in, w_out.T, mod_scale, mod_shift,
            step_size.reshape(1, per_dev),
        )
        return out.transpose(0, 1, 3, 2)

    return jax.shard_map(
        local_run,
        mesh=mesh,
        in_specs=(P(("part", "data"), None, None), P(None, None), P(None, None), P("time", None), P("time", None), P("time")),
        out_specs=P("time", ("part", "data"), None, None),
        check_vma=False,
    )
```

```python
import functools
import math

import jax
import jax.numpy as jnp
from jax import lax
from jax.experimental import pallas as pl
from jax.experimental.pallas import tpu as pltpu
from jax.sharding import PartitionSpec as P

SWEEPS = 4
ROWS = 128
LANES = 128
AHEAD = 5
BEHIND = 1
MESH = pl.DeviceIdType.MESH

A = 2.0 * math.sqrt(2.0 / math.pi)
B = 8.0 * math.sqrt(2.0 / math.pi) * 0.044715


def kernel(
    x_hbm, win_hbm, wout_hbm, scale_hbm, shift_hbm, step_hbm, out_ref,
    xs, win, wout, mods, scales, steps, weights, drifts, sums, sums_in, base_out, base_in, last_in,
    local_sem, pair_send, pair_recv, base_send, base_recv, last_send, last_recv, ready,
):
    me = lax.axis_index("time")
    chip, core = me // 2, lax.rem(me, 2)
    partner = 2 * chip + 1 - core
    far = 3 - me
    side = 2 * (1 - chip) + core
    sample = lax.rem(core + chip, 2)
    per_dev = mods.shape[2]
    hidden = win.shape[1]
    held = 2 * per_dev
    pairs = per_dev // 2

    barrier = pltpu.get_barrier_semaphore()
    pl.semaphore_signal(barrier, inc=1, device_id={"time": partner}, device_id_type=MESH)

    @pl.when(chip == 0)
    def _():
        for peer in (far, side):
            pl.semaphore_signal(barrier, inc=1, device_id={"time": peer}, device_id_type=MESH)

    loads = [
        pltpu.make_async_copy(source, target, local_sem.at[at])
        for at, (source, target) in enumerate((
            (scale_hbm, mods.at[core, 0]), (shift_hbm, mods.at[core, 1]), (step_hbm, steps.at[core]),
            (win_hbm, win), (x_hbm, xs), (wout_hbm, wout)))
    ]
    for load in loads:
        load.start()
    for load in loads[:3]:
        load.wait()
    pl.semaphore_wait(barrier, 1 + 2 * chip)

    def swap(at, ref, source):
        return pltpu.make_async_remote_copy(
            src_ref=ref.at[source], dst_ref=ref.at[source], send_sem=pair_send.at[at], recv_sem=pair_recv.at[at],
            device_id={"time": partner}, device_id_type=MESH)

    for at, ref in enumerate((mods, steps)):
        swap(at, ref, core).start()

    @pl.when(chip == 1)
    def _():
        for peer in (far, side):
            pl.semaphore_signal(ready.at[core], inc=1, device_id={"time": peer}, device_id_type=MESH)

    for load in loads[3:]:
        load.wait()

    def run(tasks):
        todo = [(task, at) for task in tasks for at in range(0, hidden, ROWS)]
        halves, acts, right, total = {}, {}, {}, {}

        def first(step):
            task, at = todo[step]
            if at == 0:
                right[id(task)] = task[1]()
            halves[step] = jnp.dot(
                weights[task[0], at:at + ROWS, :], right[id(task)], preferred_element_type=jnp.float32)

        def second(step):
            task, at = todo[step]
            part = jnp.dot(wout[:, at:at + ROWS], acts.pop(step), preferred_element_type=jnp.float32)
            total[id(task)] = part if at == 0 else total[id(task)] + part
            if at + ROWS == hidden:
                task[2](total[id(task)])

        for step in range(min(AHEAD, len(todo))):
            first(step)
        for step in range(len(todo)):
            if step + AHEAD < len(todo):
                first(step + AHEAD)
            half = halves.pop(step)
            arg = half * (half * half * B + A)
            acts[step] = (half * jnp.tanh(arg) + half).astype(jnp.bfloat16)
            if step >= BEHIND:
                second(step - BEHIND)
        for step in range(max(len(todo) - BEHIND, 0), len(todo)):
            second(step)

    def column(latent, index):
        half = (latent * 0.5).astype(jnp.bfloat16)
        row = lax.broadcasted_iota(jnp.int32, half.shape, 0)
        unit = jnp.where(row == index % per_dev, 0.5, 0.0).astype(jnp.bfloat16)
        blank = [jnp.zeros_like(half)] * 4
        own = [half, half, half, unit]
        return jnp.concatenate(own + blank if index % 2 == 0 else blank + own, axis=0)

    def beside(left, right):
        return jnp.concatenate([left, right], axis=1)

    def step_of(index, part=None):
        part = index // per_dev if part is None else part
        at = index % per_dev
        return jnp.broadcast_to(steps[part][:, at:at + 1], (xs.shape[1], LANES))

    def prepare(part):
        wide = win[...].astype(jnp.float32)
        scales[part] = mods[part, 0].astype(jnp.float32)
        shifts = jnp.concatenate(
            [mods[part, 1], jnp.zeros((wide.shape[0] - per_dev, hidden), jnp.bfloat16)], axis=0)
        for pair in range(pairs):
            rows = []
            for at in (2 * pair, 2 * pair + 1):
                scaled = wide * jnp.broadcast_to(scales[part, at:at + 1, :], wide.shape)
                high = scaled.astype(jnp.bfloat16)
                low = (scaled - high.astype(jnp.float32)).astype(jnp.bfloat16)
                rows += [win[...], high, low, shifts]
            weights[part * pairs + pair] = jnp.concatenate(rows, axis=0).T

    def start_of(half):
        return xs[sample, :, half * LANES:(half + 1) * LANES]

    other = 1 - core
    found = {}
    total_of = {}

    def drift_at(sweep, half, index):
        key = (sweep, half, index)
        return found[key] if key in found else drifts[half, index]

    def sum_before(sweep, half, index, settled):
        key = (sweep, half, index)
        if index == 0:
            return None
        if sweep > 0 and settled and index <= sweep:
            return sum_before(sweep - 1, half, index, settled)
        if key not in total_of:
            before = sum_before(sweep, half, index - 1, settled)
            drift = drift_at(sweep, half, index - 1)
            total_of[key] = drift if before is None else before + drift
        return total_of[key]

    def opening(done):
        def task(part, pair, half, fresh, last):
            def right():
                if fresh:
                    if part is other:
                        for at, ref in enumerate((mods, steps)):
                            swap(at, ref, other).wait_recv()
                    prepare(part)
                return beside(column(start_of(half), 2 * pair), column(start_of(half), 2 * pair + 1))

            def finish(total):
                for at in range(2):
                    index = 2 * pair + at
                    drifts[half, part * per_dev + index] = (
                        total[:, at * LANES:(at + 1) * LANES] * step_of(index, part))
                if last:
                    done(half)

            return (part * pairs + pair, right, finish)

        return [
            task(part, pair, half, half == 0 and pair == 0, part is other and pair == pairs - 1)
            for half in range(2) for part in (core, other) for pair in range(pairs)
        ]

    def add(base, part):
        return base if part is None else base + part

    def whole(sweep, index, latent, done=None):
        def finish(total):
            for half in range(2):
                found[sweep, half, index] = total[:, half * LANES:(half + 1) * LANES] * step_of(index)
            if done is not None:
                done()

        return (
            index // 2, lambda: beside(*[column(latent(sweep - 1, half, index), index) for half in range(2)]), finish)

    def paired(sweep, pair, half, latent, done=None):
        def finish(total):
            for at in range(2):
                found[sweep, half, 2 * pair + at] = total[:, at * LANES:(at + 1) * LANES] * step_of(2 * pair + at)
            if done is not None:
                done()

        return (
            pair, lambda: beside(*[column(latent(sweep - 1, half, 2 * pair + at), 2 * pair + at) for at in range(2)]),
            finish)

    def base_copy(sweep, half):
        place = (sweep, slice(None), pl.ds(half * LANES, LANES))
        return pltpu.make_async_remote_copy(
            src_ref=base_out.at[place], dst_ref=base_in.at[place], send_sem=base_send.at[2 * sweep + half],
            recv_sem=base_recv.at[2 * sweep + half], device_id={"time": far}, device_id_type=MESH)

    def last_copy(at, source):
        return pltpu.make_async_remote_copy(
            src_ref=base_out.at[SWEEPS - 1], dst_ref=last_in.at[source], send_sem=last_send.at[at],
            recv_sem=last_recv.at[source], device_id={"time": (far, side)[at]}, device_id_type=MESH)

    def sums_copy():
        return pltpu.make_async_remote_copy(
            src_ref=sums.at[pl.ds((1 - core) * per_dev, per_dev)], dst_ref=sums_in, send_sem=pair_send.at[2],
            recv_sem=pair_recv.at[2], device_id={"time": partner}, device_id_type=MESH)

    def share(settled):
        for index in range(held):
            for half in range(2):
                value = sum_before(SWEEPS - 1, half, index, settled)
                sums[index, :, half * LANES:(half + 1) * LANES] = (
                    jnp.zeros((xs.shape[1], LANES), jnp.float32) if value is None else value)
        sums_copy().start()

    def close(bases):
        out_ref[:, sample] = bases[sample] + sums[pl.ds(core * per_dev, per_dev)]
        sums_copy().wait_recv()
        out_ref[:, 1 - sample] = bases[1 - sample] + sums_in[...]

    @pl.when(chip == 0)
    def _():
        found.clear(), total_of.clear()

        def latent(sweep, half, index):
            return add(start_of(half), sum_before(sweep, half, index, True))

        def put(sweep, half):
            base_out[sweep, :, half * LANES:(half + 1) * LANES] = latent(sweep, half, held)

        def send(sweep, half):
            put(sweep, half)
            if sweep == half == 0:
                pl.semaphore_wait(ready.at[1 - core], 1)
            base_copy(sweep, half).start()

        def send_last():
            put(SWEEPS - 1, 0), put(SWEEPS - 1, 1)
            pl.semaphore_wait(ready.at[core], 1)
            for at in range(2):
                last_copy(at, sample).start()

        tasks = opening(lambda half: send(0, half))
        for sweep in range(1, SWEEPS - 1):
            odd = sweep % 2 == 1
            for half in range(2):
                many = list(range((sweep + 1) // 2, held // 2))
                for pair in many:
                    close_now = pair == many[-1] and not (odd and half == 0)
                    tasks.append(paired(
                        sweep, pair, half, latent, functools.partial(send, sweep, half) if close_now else None))
                if odd and half == 0:
                    tasks.append(whole(sweep, sweep, latent, functools.partial(send, sweep, half)))
        tasks += [
            whole(SWEEPS - 1, index, latent, send_last if index == held - 1 else None)
            for index in range(SWEEPS - 1, held)]
        run(tasks)
        share(True)
        close(xs)
        for sweep in range(SWEEPS - 1):
            for half in range(2):
                base_copy(sweep, half).wait_send()
        for at in range(2):
            last_copy(at, sample).wait_send()

    @pl.when(chip == 1)
    def _():
        found.clear(), total_of.clear()
        arrived = set()

        def latent(sweep, half, index):
            if sweep < 0:
                return start_of(half)
            if (sweep, half) not in arrived:
                arrived.add((sweep, half))
                base_copy(sweep, half).wait_recv()
            base = base_in[sweep, :, half * LANES:(half + 1) * LANES]
            return add(base, sum_before(sweep, half, index, False))

        for at, ref in enumerate((mods, steps)):
            swap(at, ref, other).wait_recv()
        prepare(0)
        prepare(1)
        tasks = []
        for sweep in range(SWEEPS):
            live = per_dev + sweep
            tasks += [paired(sweep, pair, half, latent) for half in range(2) for pair in range(live // 2)]
            if live % 2 == 1:
                tasks.append(whole(sweep, live - 1, latent))
        run(tasks)
        share(False)
        for source in range(2):
            last_copy(0, source).wait_recv()
        close(last_in)

    for at, ref in enumerate((mods, steps)):
        swap(at, ref, core).wait_send()
    sums_copy().wait_send()


def solution(mesh):
    def local_run(x_init, w_in, w_out, mod_scale, mod_shift, step_size):
        samples, tokens, channels = x_init.shape
        per_dev, hidden = mod_scale.shape
        held = 2 * per_dev
        operands = (
            x_init.transpose(0, 2, 1), w_in, w_out.T, mod_scale, mod_shift, step_size.reshape(1, per_dev))
        latent = (channels, tokens)
        out = pl.pallas_call(
            kernel,
            out_shape=pltpu.VMEM((per_dev, samples) + latent, jnp.float32),
            in_specs=[pl.BlockSpec(memory_space=pl.ANY)] * len(operands),
            out_specs=pl.BlockSpec(memory_space=pltpu.VMEM),
            scratch_shapes=[
                pltpu.VMEM((samples,) + latent, jnp.float32),
                pltpu.VMEM((channels, hidden), jnp.bfloat16),
                pltpu.VMEM((channels, hidden), jnp.bfloat16),
                pltpu.VMEM((2, 2, per_dev, hidden), jnp.bfloat16),
                pltpu.VMEM((2, per_dev, hidden), jnp.float32),
                pltpu.VMEM((2, 1, per_dev), jnp.float32),
                pltpu.VMEM((per_dev, hidden, LANES), jnp.bfloat16),
                pltpu.VMEM((2, held, channels, LANES), jnp.float32),
                pltpu.VMEM((held,) + latent, jnp.float32),
                pltpu.VMEM((per_dev,) + latent, jnp.float32),
                pltpu.VMEM((SWEEPS,) + latent, jnp.float32),
                pltpu.VMEM((SWEEPS - 1,) + latent, jnp.float32),
                pltpu.VMEM((samples,) + latent, jnp.float32),
                pltpu.SemaphoreType.DMA((6,)),
                pltpu.SemaphoreType.DMA((3,)),
                pltpu.SemaphoreType.DMA((3,)),
                pltpu.SemaphoreType.DMA((2 * SWEEPS - 2,)),
                pltpu.SemaphoreType.DMA((2 * SWEEPS - 2,)),
                pltpu.SemaphoreType.DMA((2,)),
                pltpu.SemaphoreType.DMA((2,)),
                pltpu.SemaphoreType.REGULAR((2,)),
            ],
            compiler_params=pltpu.CompilerParams(
                collective_id=0, has_side_effects=True, vmem_limit_bytes=32 << 20),
        )(*[pltpu.with_memory_space_constraint(operand, pltpu.HBM) for operand in operands])
        return out.transpose(0, 1, 3, 2)

    return jax.shard_map(
        local_run,
        mesh=mesh,
        in_specs=(P(("part", "data"), None, None), P(None, None), P(None, None), P("time", None), P("time", None), P("time")),
        out_specs=P("time", ("part", "data"), None, None),
        check_vma=False,
    )
```

```python
import functools
import math

import jax
import jax.numpy as jnp
from jax import lax
from jax.experimental import pallas as pl
from jax.experimental.pallas import tpu as pltpu
from jax.sharding import PartitionSpec as P

SWEEPS = 4
ROWS = 192
LANES = 128
AHEAD = 3
BEHIND = 1
MESH = pl.DeviceIdType.MESH

A = 2.0 * math.sqrt(2.0 / math.pi)
B = 8.0 * math.sqrt(2.0 / math.pi) * 0.044715


def kernel(
    x_hbm, win_hbm, wout_hbm, scale_hbm, shift_hbm, step_hbm, out_ref,
    xs, win, wout, mods, scales, steps, weights, drifts, sums, sums_in, base_out, base_in, last_in, hand_out, hand_in,
    local_sem, pair_send, pair_recv, base_send, base_recv, last_send, last_recv, ready,
):
    me = lax.axis_index("time")
    chip, core = me // 2, lax.rem(me, 2)
    partner = 2 * chip + 1 - core
    far = 3 - me
    side = 2 * (1 - chip) + core
    sample = lax.rem(core + chip, 2)
    per_dev = mods.shape[2]
    hidden = win.shape[1]
    held = 2 * per_dev
    pairs = per_dev // 2

    barrier = pltpu.get_barrier_semaphore()
    pl.semaphore_signal(barrier, inc=1, device_id={"time": partner}, device_id_type=MESH)

    @pl.when(chip == 0)
    def _():
        for peer in (far, side):
            pl.semaphore_signal(barrier, inc=1, device_id={"time": peer}, device_id_type=MESH)

    loads = [
        pltpu.make_async_copy(source, target, local_sem.at[at])
        for at, (source, target) in enumerate((
            (scale_hbm, mods.at[core, 0]), (shift_hbm, mods.at[core, 1]), (step_hbm, steps.at[core]),
            (win_hbm, win), (x_hbm, xs), (wout_hbm, wout)))
    ]
    for load in loads:
        load.start()
    for load in loads[:3]:
        load.wait()
    pl.semaphore_wait(barrier, 1 + 2 * chip)

    def swap(at, ref, source):
        return pltpu.make_async_remote_copy(
            src_ref=ref.at[source], dst_ref=ref.at[source], send_sem=pair_send.at[at], recv_sem=pair_recv.at[at],
            device_id={"time": partner}, device_id_type=MESH)

    for at, ref in enumerate((mods, steps)):
        swap(at, ref, core).start()

    @pl.when(chip == 1)
    def _():
        for peer in (far, side):
            pl.semaphore_signal(ready.at[core], inc=1, device_id={"time": peer}, device_id_type=MESH)

    for load in loads[3:]:
        load.wait()

    def run(tasks):
        todo = [(task, at) for task in tasks for at in range(0, hidden, ROWS)]
        halves, acts, right, total = {}, {}, {}, {}

        def first(step):
            task, at = todo[step]
            if at == 0:
                right[id(task)] = task[1]()
            halves[step] = jnp.dot(
                weights[task[0], at:at + ROWS, :], right[id(task)], preferred_element_type=jnp.float32)

        def second(step):
            task, at = todo[step]
            part = jnp.dot(wout[:, at:at + ROWS], acts.pop(step), preferred_element_type=jnp.float32)
            total[id(task)] = part if at == 0 else total[id(task)] + part
            if at + ROWS == hidden:
                task[2](total[id(task)])

        for step in range(min(AHEAD, len(todo))):
            first(step)
        for step in range(len(todo)):
            if step + AHEAD < len(todo):
                first(step + AHEAD)
            half = halves.pop(step)
            arg = half * (half * half * B + A)
            acts[step] = (half * jnp.tanh(arg) + half).astype(jnp.bfloat16)
            if step >= BEHIND:
                second(step - BEHIND)
        for step in range(max(len(todo) - BEHIND, 0), len(todo)):
            second(step)

    def column(latent, index):
        half = (latent * 0.5).astype(jnp.bfloat16)
        row = lax.broadcasted_iota(jnp.int32, half.shape, 0)
        unit = jnp.where(row == index % per_dev, 0.5, 0.0).astype(jnp.bfloat16)
        blank = [jnp.zeros_like(half)] * 4
        own = [half, half, half, unit]
        return jnp.concatenate(own + blank if index % 2 == 0 else blank + own, axis=0)

    def beside(left, right):
        return jnp.concatenate([left, right], axis=1)

    def step_of(index, part=None):
        part = index // per_dev if part is None else part
        at = index % per_dev
        return jnp.broadcast_to(steps[part][:, at:at + 1], (xs.shape[1], LANES))

    def prepare(part):
        wide = win[...].astype(jnp.float32)
        scales[part] = mods[part, 0].astype(jnp.float32)
        shifts = jnp.concatenate(
            [mods[part, 1], jnp.zeros((wide.shape[0] - per_dev, hidden), jnp.bfloat16)], axis=0)
        for pair in range(pairs):
            rows = []
            for at in (2 * pair, 2 * pair + 1):
                scaled = wide * jnp.broadcast_to(scales[part, at:at + 1, :], wide.shape)
                high = scaled.astype(jnp.bfloat16)
                low = (scaled - high.astype(jnp.float32)).astype(jnp.bfloat16)
                rows += [win[...], high, low, shifts]
            weights[part * pairs + pair] = jnp.concatenate(rows, axis=0).T

    def start_of(half):
        return xs[sample, :, half * LANES:(half + 1) * LANES]

    other = 1 - core
    found = {}
    total_of = {}

    def drift_at(sweep, half, index):
        key = (sweep, half, index)
        return found[key] if key in found else drifts[half, index]

    def sum_before(sweep, half, index, settled):
        key = (sweep, half, index)
        if index == 0:
            return None
        if sweep > 0 and settled and index <= sweep:
            return sum_before(sweep - 1, half, index, settled)
        if key not in total_of:
            before = sum_before(sweep, half, index - 1, settled)
            drift = drift_at(sweep, half, index - 1)
            total_of[key] = drift if before is None else before + drift
        return total_of[key]

    def opening(done):
        def task(part, pair, half, fresh, last):
            def right():
                if fresh:
                    if part is other:
                        for at, ref in enumerate((mods, steps)):
                            swap(at, ref, other).wait_recv()
                    prepare(part)
                return beside(column(start_of(half), 2 * pair), column(start_of(half), 2 * pair + 1))

            def finish(total):
                for at in range(2):
                    index = 2 * pair + at
                    drifts[half, part * per_dev + index] = (
                        total[:, at * LANES:(at + 1) * LANES] * step_of(index, part))
                if last:
                    done(half)

            return (part * pairs + pair, right, finish)

        return [
            task(part, pair, half, half == 0 and pair == 0, part is other and pair == pairs - 1)
            for half in range(2) for part in (core, other) for pair in range(pairs)
        ]

    def add(base, part):
        return base if part is None else base + part

    def whole(sweep, index, latent, done=None):
        def finish(total):
            for half in range(2):
                found[sweep, half, index] = total[:, half * LANES:(half + 1) * LANES] * step_of(index)
            if done is not None:
                done()

        return (
            index // 2, lambda: beside(*[column(latent(sweep - 1, half, index), index) for half in range(2)]), finish)

    def paired(sweep, pair, half, latent, done=None):
        def finish(total):
            for at in range(2):
                found[sweep, half, 2 * pair + at] = total[:, at * LANES:(at + 1) * LANES] * step_of(2 * pair + at)
            if done is not None:
                done()

        return (
            pair, lambda: beside(*[column(latent(sweep - 1, half, 2 * pair + at), 2 * pair + at) for at in range(2)]),
            finish)

    def base_copy(sweep, half):
        place = (sweep, slice(None), pl.ds(half * LANES, LANES))
        return pltpu.make_async_remote_copy(
            src_ref=base_out.at[place], dst_ref=base_in.at[place], send_sem=base_send.at[2 * sweep + half],
            recv_sem=base_recv.at[2 * sweep + half], device_id={"time": far}, device_id_type=MESH)

    def last_copy(at, source, half):
        lanes = pl.ds(half * LANES, LANES)
        return pltpu.make_async_remote_copy(
            src_ref=base_out.at[SWEEPS - 1, :, lanes], dst_ref=last_in.at[source, :, lanes],
            send_sem=last_send.at[2 * at + half], recv_sem=last_recv.at[2 * source + half],
            device_id={"time": (far, side)[at]}, device_id_type=MESH)

    def sums_copy(start, count):
        return pltpu.make_async_remote_copy(
            src_ref=sums.at[pl.ds(start, count)], dst_ref=sums_in.at[pl.ds(0, count)], send_sem=pair_send.at[2],
            recv_sem=pair_recv.at[2], device_id={"time": partner}, device_id_type=MESH)

    def hand_copy():
        return pltpu.make_async_remote_copy(
            src_ref=hand_out, dst_ref=hand_in, send_sem=pair_send.at[3],
            recv_sem=pair_recv.at[3], device_id={"time": partner}, device_id_type=MESH)

    def whole_sum(index, settled):
        values = [sum_before(SWEEPS - 1, half, index, settled) for half in range(2)]
        if values[0] is None:
            return jnp.zeros(xs.shape[1:], jnp.float32)
        return beside(*values)

    @pl.when(chip == 0)
    def _():
        found.clear(), total_of.clear()

        def latent(sweep, half, index):
            return add(start_of(half), sum_before(sweep, half, index, True))

        def put(sweep, half):
            base_out[sweep, :, half * LANES:(half + 1) * LANES] = latent(sweep, half, held)

        def send(sweep, half):
            put(sweep, half)
            if sweep == half == 0:
                pl.semaphore_wait(ready.at[1 - core], 1)
            base_copy(sweep, half).start()

        def send_last(half):
            put(SWEEPS - 1, half)
            if half == 0:
                pl.semaphore_wait(ready.at[core], 1)
            for at in range(2):
                last_copy(at, sample, half).start()

        tasks = opening(lambda half: send(0, half))
        for sweep in range(1, SWEEPS - 1):
            odd = sweep % 2 == 1
            for half in range(2):
                many = list(range((sweep + 1) // 2, held // 2))
                for pair in many:
                    close_now = pair == many[-1] and not (odd and half == 0)
                    tasks.append(paired(
                        sweep, pair, half, latent, functools.partial(send, sweep, half) if close_now else None))
                if odd and half == 0:
                    tasks.append(whole(sweep, sweep, latent, functools.partial(send, sweep, half)))
        tasks.append(whole(SWEEPS - 1, SWEEPS - 1, latent))
        for half in range(2):
            for pair in range(SWEEPS // 2, held // 2):
                tasks.append(paired(
                    SWEEPS - 1, pair, half, latent,
                    functools.partial(send_last, half) if pair == held // 2 - 1 else None))
        run(tasks)
        for index in range(held):
            sums[index] = whole_sum(index, True)
        sums_copy(other * per_dev, per_dev).start()
        out_ref[:, sample] = xs[sample] + sums[pl.ds(core * per_dev, per_dev)]
        sums_copy(0, per_dev).wait_recv()
        out_ref[:, 1 - sample] = xs[1 - sample] + sums_in[...]
        for sweep in range(SWEEPS - 1):
            for half in range(2):
                base_copy(sweep, half).wait_send()
        for at in range(2):
            for half in range(2):
                last_copy(at, sample, half).wait_send()
        sums_copy(0, per_dev).wait_send()

    def second_chip(which):
        found.clear(), total_of.clear()
        arrived = set()
        mine, theirs = (1 + which) % 2, which % 2
        last = SWEEPS - 1
        lent = {}

        def latent(sweep, half, index):
            if sweep < 0:
                return start_of(half)
            if (sweep, half) not in arrived:
                arrived.add((sweep, half))
                base_copy(sweep, half).wait_recv()
            base = base_in[sweep, :, half * LANES:(half + 1) * LANES]
            return add(base, sum_before(sweep, half, index, False))

        def hand():
            for half in range(2):
                hand_out[:, half * LANES:(half + 1) * LANES] = latent(last - 1, half, held - 2)
            hand_copy().start()

        def early():
            for index in range(per_dev):
                sums[index] = whole_sum(index, False)
            sums_copy(0, per_dev).start()

        def extra():
            def right():
                hand_copy().wait_recv()
                return beside(*[
                    column(hand_in[:, half * LANES:(half + 1) * LANES], held - 2) for half in range(2)])

            def finish(total):
                lent[0] = total * beside(step_of(held - 2), step_of(held - 2))

            return (held // 2 - 1, right, finish)

        for at, ref in enumerate((mods, steps)):
            swap(at, ref, other).wait_recv()
        prepare(0)
        prepare(1)
        tasks = []
        for sweep in range(SWEEPS):
            live = per_dev + sweep
            for half in range(2):
                for pair in range(live // 2):
                    done = None
                    if sweep == last and half == 1 and pair == 0 and which == 0:
                        done = hand
                    if sweep == last and half == 1 and pair == per_dev // 2 - 1 and which == 1:
                        done = early
                    tasks.append(paired(sweep, pair, half, latent, done))
            if live % 2 == 1 and not (sweep == last and which == 0):
                tasks.append(whole(sweep, live - 1, latent))
        if which == 1:
            tasks.append(extra())
        run(tasks)
        if which == 0:
            for index in range(per_dev, held - 1):
                sums[index] = whole_sum(index, False)
            sums_copy(per_dev, per_dev - 1).start()
        for source in range(2):
            for half in range(2):
                last_copy(0, source, half).wait_recv()
        for index in range(per_dev):
            out_ref[index, mine] = last_in[mine] + whole_sum(which * per_dev + index, False)
        if which == 0:
            sums_copy(0, per_dev).wait_recv()
            out_ref[:, theirs] = last_in[theirs] + sums_in[...]
            hand_copy().wait_send()
            sums_copy(0, per_dev - 1).wait_send()
        else:
            sums_copy(0, per_dev - 1).wait_recv()
            out_ref[:per_dev - 1, theirs] = last_in[theirs] + sums_in[:per_dev - 1]
            out_ref[per_dev - 1, theirs] = last_in[theirs] + (sums_in[per_dev - 2] + lent[0])
            sums_copy(0, per_dev).wait_send()

    for which in range(2):
        @pl.when(me == 2 + which)
        def _():
            second_chip(which)

    for at, ref in enumerate((mods, steps)):
        swap(at, ref, core).wait_send()


def solution(mesh):
    def local_run(x_init, w_in, w_out, mod_scale, mod_shift, step_size):
        samples, tokens, channels = x_init.shape
        per_dev, hidden = mod_scale.shape
        held = 2 * per_dev
        operands = (
            x_init.transpose(0, 2, 1), w_in, w_out.T, mod_scale, mod_shift, step_size.reshape(1, per_dev))
        latent = (channels, tokens)
        out = pl.pallas_call(
            kernel,
            out_shape=pltpu.VMEM((per_dev, samples) + latent, jnp.float32),
            in_specs=[pl.BlockSpec(memory_space=pl.ANY)] * len(operands),
            out_specs=pl.BlockSpec(memory_space=pltpu.VMEM),
            scratch_shapes=[
                pltpu.VMEM((samples,) + latent, jnp.float32),
                pltpu.VMEM((channels, hidden), jnp.bfloat16),
                pltpu.VMEM((channels, hidden), jnp.bfloat16),
                pltpu.VMEM((2, 2, per_dev, hidden), jnp.bfloat16),
                pltpu.VMEM((2, per_dev, hidden), jnp.float32),
                pltpu.VMEM((2, 1, per_dev), jnp.float32),
                pltpu.VMEM((per_dev, hidden, LANES), jnp.bfloat16),
                pltpu.VMEM((2, held, channels, LANES), jnp.float32),
                pltpu.VMEM((held,) + latent, jnp.float32),
                pltpu.VMEM((per_dev,) + latent, jnp.float32),
                pltpu.VMEM((SWEEPS,) + latent, jnp.float32),
                pltpu.VMEM((SWEEPS - 1,) + latent, jnp.float32),
                pltpu.VMEM((samples,) + latent, jnp.float32),
                pltpu.VMEM(latent, jnp.float32),
                pltpu.VMEM(latent, jnp.float32),
                pltpu.SemaphoreType.DMA((6,)),
                pltpu.SemaphoreType.DMA((4,)),
                pltpu.SemaphoreType.DMA((4,)),
                pltpu.SemaphoreType.DMA((2 * SWEEPS - 2,)),
                pltpu.SemaphoreType.DMA((2 * SWEEPS - 2,)),
                pltpu.SemaphoreType.DMA((4,)),
                pltpu.SemaphoreType.DMA((4,)),
                pltpu.SemaphoreType.REGULAR((2,)),
            ],
            compiler_params=pltpu.CompilerParams(
                collective_id=0, has_side_effects=True, vmem_limit_bytes=32 << 20),
        )(*[pltpu.with_memory_space_constraint(operand, pltpu.HBM) for operand in operands])
        return out.transpose(0, 1, 3, 2)

    return jax.shard_map(
        local_run,
        mesh=mesh,
        in_specs=(P(("part", "data"), None, None), P(None, None), P(None, None), P("time", None), P("time", None), P("time")),
        out_specs=P("time", ("part", "data"), None, None),
        check_vma=False,
    )
```

```python
import functools
import math

import jax
import jax.numpy as jnp
from jax import lax
from jax.experimental import pallas as pl
from jax.experimental.pallas import tpu as pltpu
from jax.sharding import PartitionSpec as P

SWEEPS = 4
ROWS = 256
LANES = 128
AHEAD = 3
BEHIND = 1
MESH = pl.DeviceIdType.MESH

A = 2.0 * math.sqrt(2.0 / math.pi)
B = 8.0 * math.sqrt(2.0 / math.pi) * 0.044715


def kernel(
    x_hbm, win_hbm, wout_hbm, scale_hbm, shift_hbm, step_hbm, out_ref,
    xs, win, wout, mods, scales, steps, weights, drifts, sums, sums_in, base_out, base_in, last_in, hand_out, hand_in,
    local_sem, pair_send, pair_recv, base_send, base_recv, last_send, last_recv, ready,
):
    me = lax.axis_index("time")
    chip, core = me // 2, lax.rem(me, 2)
    partner = 2 * chip + 1 - core
    far = 3 - me
    side = 2 * (1 - chip) + core
    sample = lax.rem(core + chip, 2)
    per_dev = mods.shape[2]
    hidden = win.shape[1]
    held = 2 * per_dev
    pairs = per_dev // 2

    barrier = pltpu.get_barrier_semaphore()
    pl.semaphore_signal(barrier, inc=1, device_id={"time": partner}, device_id_type=MESH)

    @pl.when(chip == 0)
    def _():
        for peer in (far, side):
            pl.semaphore_signal(barrier, inc=1, device_id={"time": peer}, device_id_type=MESH)

    loads = [
        pltpu.make_async_copy(source, target, local_sem.at[at])
        for at, (source, target) in enumerate((
            (scale_hbm, mods.at[core, 0]), (shift_hbm, mods.at[core, 1]), (step_hbm, steps.at[core]),
            (win_hbm, win), (x_hbm, xs), (wout_hbm, wout)))
    ]
    for load in loads:
        load.start()
    for load in loads[:3]:
        load.wait()
    pl.semaphore_wait(barrier, 1 + 2 * chip)

    def swap(at, ref, source):
        return pltpu.make_async_remote_copy(
            src_ref=ref.at[source], dst_ref=ref.at[source], send_sem=pair_send.at[at], recv_sem=pair_recv.at[at],
            device_id={"time": partner}, device_id_type=MESH)

    for at, ref in enumerate((mods, steps)):
        swap(at, ref, core).start()

    @pl.when(chip == 1)
    def _():
        for peer in (far, side):
            pl.semaphore_signal(ready.at[core], inc=1, device_id={"time": peer}, device_id_type=MESH)

    for load in loads[3:]:
        load.wait()

    def run(tasks):
        todo = [(task, slice(at, min(at + ROWS, hidden))) for task in tasks for at in range(0, hidden, ROWS)]
        halves, acts, right, total = {}, {}, {}, {}

        def first(step):
            task, at = todo[step]
            if at.start == 0:
                right[id(task)] = task[1]()
            halves[step] = jnp.dot(
                weights[task[0], at, :], right[id(task)], preferred_element_type=jnp.float32)

        def second(step):
            task, at = todo[step]
            part = jnp.dot(wout[:, at], acts.pop(step), preferred_element_type=jnp.float32)
            total[id(task)] = part if at.start == 0 else total[id(task)] + part
            if at.stop == hidden:
                task[2](total[id(task)])

        for step in range(min(AHEAD, len(todo))):
            first(step)
        for step in range(len(todo)):
            if step + AHEAD < len(todo):
                first(step + AHEAD)
            half = halves.pop(step)
            arg = half * (half * half * B + A)
            acts[step] = (half * jnp.tanh(arg) + half).astype(jnp.bfloat16)
            if step >= BEHIND:
                second(step - BEHIND)
        for step in range(max(len(todo) - BEHIND, 0), len(todo)):
            second(step)

    def column(latent, index):
        half = (latent * 0.5).astype(jnp.bfloat16)
        row = lax.broadcasted_iota(jnp.int32, half.shape, 0)
        unit = jnp.where(row == index % per_dev, 0.5, 0.0).astype(jnp.bfloat16)
        blank = [jnp.zeros_like(half)] * 4
        own = [half, half, half, unit]
        return jnp.concatenate(own + blank if index % 2 == 0 else blank + own, axis=0)

    def beside(left, right):
        return jnp.concatenate([left, right], axis=1)

    def step_of(index, part=None):
        part = index // per_dev if part is None else part
        at = index % per_dev
        return jnp.broadcast_to(steps[part][:, at:at + 1], (xs.shape[1], LANES))

    def prepare(part):
        wide = win[...].astype(jnp.float32)
        scales[part] = mods[part, 0].astype(jnp.float32)
        shifts = jnp.concatenate(
            [mods[part, 1], jnp.zeros((wide.shape[0] - per_dev, hidden), jnp.bfloat16)], axis=0)
        for pair in range(pairs):
            rows = []
            for at in (2 * pair, 2 * pair + 1):
                scaled = wide * jnp.broadcast_to(scales[part, at:at + 1, :], wide.shape)
                high = scaled.astype(jnp.bfloat16)
                low = (scaled - high.astype(jnp.float32)).astype(jnp.bfloat16)
                rows += [win[...], high, low, shifts]
            weights[part * pairs + pair] = jnp.concatenate(rows, axis=0).T

    def start_of(half):
        return xs[sample, :, half * LANES:(half + 1) * LANES]

    other = 1 - core
    found = {}
    total_of = {}

    def drift_at(sweep, half, index):
        key = (sweep, half, index)
        return found[key] if key in found else drifts[half, index]

    def sum_before(sweep, half, index, settled):
        key = (sweep, half, index)
        if index == 0:
            return None
        if sweep > 0 and settled and index <= sweep:
            return sum_before(sweep - 1, half, index, settled)
        if key not in total_of:
            before = sum_before(sweep, half, index - 1, settled)
            drift = drift_at(sweep, half, index - 1)
            total_of[key] = drift if before is None else before + drift
        return total_of[key]

    def opening(done):
        def task(part, pair, half, fresh, last):
            def right():
                if fresh:
                    if part is other:
                        for at, ref in enumerate((mods, steps)):
                            swap(at, ref, other).wait_recv()
                    prepare(part)
                return beside(column(start_of(half), 2 * pair), column(start_of(half), 2 * pair + 1))

            def finish(total):
                for at in range(2):
                    index = 2 * pair + at
                    drifts[half, part * per_dev + index] = (
                        total[:, at * LANES:(at + 1) * LANES] * step_of(index, part))
                if last:
                    done(half)

            return (part * pairs + pair, right, finish)

        return [
            task(part, pair, half, half == 0 and pair == 0, part is other and pair == pairs - 1)
            for part in (core, other) for half in range(2) for pair in range(pairs)
        ]

    def add(base, part):
        return base if part is None else base + part

    def whole(sweep, index, latent, done=None):
        def finish(total):
            for half in range(2):
                found[sweep, half, index] = total[:, half * LANES:(half + 1) * LANES] * step_of(index)
            if done is not None:
                done()

        return (
            index // 2, lambda: beside(*[column(latent(sweep - 1, half, index), index) for half in range(2)]), finish)

    def paired(sweep, pair, half, latent, done=None):
        def finish(total):
            for at in range(2):
                found[sweep, half, 2 * pair + at] = total[:, at * LANES:(at + 1) * LANES] * step_of(2 * pair + at)
            if done is not None:
                done()

        return (
            pair, lambda: beside(*[column(latent(sweep - 1, half, 2 * pair + at), 2 * pair + at) for at in range(2)]),
            finish)

    def base_copy(sweep, half):
        place = (sweep, slice(None), pl.ds(half * LANES, LANES))
        return pltpu.make_async_remote_copy(
            src_ref=base_out.at[place], dst_ref=base_in.at[place], send_sem=base_send.at[2 * sweep + half],
            recv_sem=base_recv.at[2 * sweep + half], device_id={"time": far}, device_id_type=MESH)

    def last_copy(at, source, half):
        lanes = pl.ds(half * LANES, LANES)
        return pltpu.make_async_remote_copy(
            src_ref=base_out.at[SWEEPS - 1, :, lanes], dst_ref=last_in.at[source, :, lanes],
            send_sem=last_send.at[2 * at + half], recv_sem=last_recv.at[2 * source + half],
            device_id={"time": (far, side)[at]}, device_id_type=MESH)

    def sums_copy(start, count):
        return pltpu.make_async_remote_copy(
            src_ref=sums.at[pl.ds(start, count)], dst_ref=sums_in.at[pl.ds(0, count)], send_sem=pair_send.at[2],
            recv_sem=pair_recv.at[2], device_id={"time": partner}, device_id_type=MESH)

    def hand_copy():
        return pltpu.make_async_remote_copy(
            src_ref=hand_out, dst_ref=hand_in, send_sem=pair_send.at[3],
            recv_sem=pair_recv.at[3], device_id={"time": partner}, device_id_type=MESH)

    def whole_sum(index, settled):
        values = [sum_before(SWEEPS - 1, half, index, settled) for half in range(2)]
        if values[0] is None:
            return jnp.zeros(xs.shape[1:], jnp.float32)
        return beside(*values)

    @pl.when(chip == 0)
    def _():
        found.clear(), total_of.clear()

        def latent(sweep, half, index):
            return add(start_of(half), sum_before(sweep, half, index, True))

        def put(sweep, half):
            base_out[sweep, :, half * LANES:(half + 1) * LANES] = latent(sweep, half, held)

        def send(sweep, half):
            put(sweep, half)
            if sweep == half == 0:
                pl.semaphore_wait(ready.at[1 - core], 1)
            base_copy(sweep, half).start()

        def send_last(half):
            put(SWEEPS - 1, half)
            if half == 0:
                pl.semaphore_wait(ready.at[core], 1)
            for at in range(2):
                last_copy(at, sample, half).start()

        tasks = opening(lambda half: send(0, half))
        for sweep in range(1, SWEEPS - 1):
            odd = sweep % 2 == 1
            for half in range(2):
                many = list(range((sweep + 1) // 2, held // 2))
                for pair in many:
                    close_now = pair == many[-1] and not (odd and half == 0)
                    tasks.append(paired(
                        sweep, pair, half, latent, functools.partial(send, sweep, half) if close_now else None))
                if odd and half == 0:
                    tasks.append(whole(sweep, sweep, latent, functools.partial(send, sweep, half)))
        tasks.append(whole(SWEEPS - 1, SWEEPS - 1, latent))
        for half in range(2):
            for pair in range(SWEEPS // 2, held // 2):
                tasks.append(paired(
                    SWEEPS - 1, pair, half, latent,
                    functools.partial(send_last, half) if pair == held // 2 - 1 else None))
        run(tasks)
        for index in range(held):
            sums[index] = whole_sum(index, True)
        sums_copy(other * per_dev, per_dev).start()
        out_ref[:, sample] = xs[sample] + sums[pl.ds(core * per_dev, per_dev)]
        sums_copy(0, per_dev).wait_recv()
        out_ref[:, 1 - sample] = xs[1 - sample] + sums_in[...]
        for sweep in range(SWEEPS - 1):
            for half in range(2):
                base_copy(sweep, half).wait_send()
        for at in range(2):
            for half in range(2):
                last_copy(at, sample, half).wait_send()
        sums_copy(0, per_dev).wait_send()

    def second_chip(which):
        found.clear(), total_of.clear()
        arrived = set()
        mine, theirs = (1 + which) % 2, which % 2
        last = SWEEPS - 1
        lent = {}

        def latent(sweep, half, index):
            if sweep < 0:
                return start_of(half)
            if (sweep, half) not in arrived:
                arrived.add((sweep, half))
                base_copy(sweep, half).wait_recv()
            base = base_in[sweep, :, half * LANES:(half + 1) * LANES]
            return add(base, sum_before(sweep, half, index, False))

        def hand():
            for half in range(2):
                hand_out[:, half * LANES:(half + 1) * LANES] = latent(last - 1, half, held - 2)
            hand_copy().start()

        def early():
            for index in range(per_dev):
                sums[index] = whole_sum(index, False)
            sums_copy(0, per_dev).start()

        def extra():
            def right():
                hand_copy().wait_recv()
                return beside(*[
                    column(hand_in[:, half * LANES:(half + 1) * LANES], held - 2) for half in range(2)])

            def finish(total):
                lent[0] = total * beside(step_of(held - 2), step_of(held - 2))

            return (held // 2 - 1, right, finish)

        for at, ref in enumerate((mods, steps)):
            swap(at, ref, other).wait_recv()
        prepare(0)
        prepare(1)
        tasks = []
        for sweep in range(SWEEPS):
            live = per_dev + sweep
            for half in range(2):
                for pair in range(live // 2):
                    done = None
                    if sweep == last and half == 1 and pair == 0 and which == 0:
                        done = hand
                    if sweep == last and half == 1 and pair == per_dev // 2 - 1 and which == 1:
                        done = early
                    tasks.append(paired(sweep, pair, half, latent, done))
            if live % 2 == 1 and not (sweep == last and which == 0):
                tasks.append(whole(sweep, live - 1, latent))
        if which == 1:
            tasks.append(extra())
        run(tasks)
        if which == 0:
            for index in range(per_dev, held - 1):
                sums[index] = whole_sum(index, False)
            sums_copy(per_dev, per_dev - 1).start()
        for source in range(2):
            for half in range(2):
                last_copy(0, source, half).wait_recv()
        for index in range(per_dev):
            out_ref[index, mine] = last_in[mine] + whole_sum(which * per_dev + index, False)
        if which == 0:
            sums_copy(0, per_dev).wait_recv()
            out_ref[:, theirs] = last_in[theirs] + sums_in[...]
            hand_copy().wait_send()
            sums_copy(0, per_dev - 1).wait_send()
        else:
            sums_copy(0, per_dev - 1).wait_recv()
            out_ref[:per_dev - 1, theirs] = last_in[theirs] + sums_in[:per_dev - 1]
            out_ref[per_dev - 1, theirs] = last_in[theirs] + (sums_in[per_dev - 2] + lent[0])
            sums_copy(0, per_dev).wait_send()

    for which in range(2):
        @pl.when(me == 2 + which)
        def _():
            second_chip(which)

    for at, ref in enumerate((mods, steps)):
        swap(at, ref, core).wait_send()


def solution(mesh):
    def local_run(x_init, w_in, w_out, mod_scale, mod_shift, step_size):
        samples, tokens, channels = x_init.shape
        per_dev, hidden = mod_scale.shape
        held = 2 * per_dev
        operands = (
            x_init.transpose(0, 2, 1), w_in, w_out.T, mod_scale, mod_shift, step_size.reshape(1, per_dev))
        latent = (channels, tokens)
        out = pl.pallas_call(
            kernel,
            out_shape=pltpu.VMEM((per_dev, samples) + latent, jnp.float32),
            in_specs=[pl.BlockSpec(memory_space=pl.ANY)] * len(operands),
            out_specs=pl.BlockSpec(memory_space=pltpu.VMEM),
            scratch_shapes=[
                pltpu.VMEM((samples,) + latent, jnp.float32),
                pltpu.VMEM((channels, hidden), jnp.bfloat16),
                pltpu.VMEM((channels, hidden), jnp.bfloat16),
                pltpu.VMEM((2, 2, per_dev, hidden), jnp.bfloat16),
                pltpu.VMEM((2, per_dev, hidden), jnp.float32),
                pltpu.VMEM((2, 1, per_dev), jnp.float32),
                pltpu.VMEM((per_dev, hidden, LANES), jnp.bfloat16),
                pltpu.VMEM((2, held, channels, LANES), jnp.float32),
                pltpu.VMEM((held,) + latent, jnp.float32),
                pltpu.VMEM((per_dev,) + latent, jnp.float32),
                pltpu.VMEM((SWEEPS,) + latent, jnp.float32),
                pltpu.VMEM((SWEEPS - 1,) + latent, jnp.float32),
                pltpu.VMEM((samples,) + latent, jnp.float32),
                pltpu.VMEM(latent, jnp.float32),
                pltpu.VMEM(latent, jnp.float32),
                pltpu.SemaphoreType.DMA((6,)),
                pltpu.SemaphoreType.DMA((4,)),
                pltpu.SemaphoreType.DMA((4,)),
                pltpu.SemaphoreType.DMA((2 * SWEEPS - 2,)),
                pltpu.SemaphoreType.DMA((2 * SWEEPS - 2,)),
                pltpu.SemaphoreType.DMA((4,)),
                pltpu.SemaphoreType.DMA((4,)),
                pltpu.SemaphoreType.REGULAR((2,)),
            ],
            compiler_params=pltpu.CompilerParams(
                collective_id=0, has_side_effects=True, vmem_limit_bytes=32 << 20),
        )(*[pltpu.with_memory_space_constraint(operand, pltpu.HBM) for operand in operands])
        return out.transpose(0, 1, 3, 2)

    return jax.shard_map(
        local_run,
        mesh=mesh,
        in_specs=(P(("part", "data"), None, None), P(None, None), P(None, None), P("time", None), P("time", None), P("time")),
        out_specs=P("time", ("part", "data"), None, None),
        check_vma=False,
    )
```

```python
import functools
import math

import jax
import jax.numpy as jnp
from jax import lax
from jax.experimental import pallas as pl
from jax.experimental.pallas import tpu as pltpu
from jax.sharding import PartitionSpec as P

SWEEPS = 4
ROWS = 256
LANES = 128
AHEAD = 3
BEHIND = 1
MESH = pl.DeviceIdType.MESH

A = 2.0 * math.sqrt(2.0 / math.pi)
B = 8.0 * math.sqrt(2.0 / math.pi) * 0.044715


def kernel(
    x_hbm, win_hbm, wout_hbm, scale_hbm, shift_hbm, step_hbm, out_ref,
    xs, win, wout, mods, scales, steps, weights, drifts, sums, sums_in, base_out, base_in, last_in, hand_out, hand_in,
    local_sem, pair_send, pair_recv, base_send, base_recv, last_send, last_recv, ready,
):
    me = lax.axis_index("time")
    chip, core = me // 2, lax.rem(me, 2)
    partner = 2 * chip + 1 - core
    far = 3 - me
    side = 2 * (1 - chip) + core
    sample = lax.rem(core + chip, 2)
    per_dev = mods.shape[2]
    hidden = win.shape[1]
    held = 2 * per_dev
    pairs = per_dev // 2

    barrier = pltpu.get_barrier_semaphore()
    pl.semaphore_signal(barrier, inc=1, device_id={"time": partner}, device_id_type=MESH)

    @pl.when(chip == 0)
    def _():
        for peer in (far, side):
            pl.semaphore_signal(barrier, inc=1, device_id={"time": peer}, device_id_type=MESH)

    loads = [
        pltpu.make_async_copy(source, target, local_sem.at[at])
        for at, (source, target) in enumerate((
            (scale_hbm, mods.at[core, 0]), (shift_hbm, mods.at[core, 1]), (step_hbm, steps.at[core]),
            (win_hbm, win), (x_hbm, xs), (wout_hbm, wout)))
    ]
    for load in loads:
        load.start()
    for load in loads[:3]:
        load.wait()
    pl.semaphore_wait(barrier, 1 + 2 * chip)

    def swap(at, ref, source):
        return pltpu.make_async_remote_copy(
            src_ref=ref.at[source], dst_ref=ref.at[source], send_sem=pair_send.at[at], recv_sem=pair_recv.at[at],
            device_id={"time": partner}, device_id_type=MESH)

    for at, ref in enumerate((mods, steps)):
        swap(at, ref, core).start()

    @pl.when(chip == 1)
    def _():
        for peer in (far, side):
            pl.semaphore_signal(ready.at[core], inc=1, device_id={"time": peer}, device_id_type=MESH)

    for load in loads[3:]:
        load.wait()

    def run(tasks):
        todo = [(task, slice(at, min(at + ROWS, hidden))) for task in tasks for at in range(0, hidden, ROWS)]
        halves, acts, right, total = {}, {}, {}, {}

        def first(step):
            task, at = todo[step]
            if at.start == 0:
                right[id(task)] = task[1]()
            halves[step] = jnp.dot(
                weights[task[0], at, :], right[id(task)], preferred_element_type=jnp.float32)

        def second(step):
            task, at = todo[step]
            part = jnp.dot(wout[:, at], acts.pop(step), preferred_element_type=jnp.float32)
            total[id(task)] = part if at.start == 0 else total[id(task)] + part
            if at.stop == hidden:
                task[2](total[id(task)])

        for step in range(min(AHEAD, len(todo))):
            first(step)
        for step in range(len(todo)):
            if step + AHEAD < len(todo):
                first(step + AHEAD)
            half = halves.pop(step)
            arg = half * (half * half * B + A)
            acts[step] = (half * jnp.tanh(arg) + half).astype(jnp.bfloat16)
            if step >= BEHIND:
                second(step - BEHIND)
        for step in range(max(len(todo) - BEHIND, 0), len(todo)):
            second(step)

    def column(latent, index):
        half = (latent * 0.5).astype(jnp.bfloat16)
        row = lax.broadcasted_iota(jnp.int32, half.shape, 0)
        unit = jnp.where(row == index % per_dev, 0.5, 0.0).astype(jnp.bfloat16)
        blank = [jnp.zeros_like(half)] * 4
        own = [half, half, half, unit]
        return jnp.concatenate(own + blank if index % 2 == 0 else blank + own, axis=0)

    def beside(left, right):
        return jnp.concatenate([left, right], axis=1)

    def step_of(index, part=None):
        part = index // per_dev if part is None else part
        at = index % per_dev
        return jnp.broadcast_to(steps[part][:, at:at + 1], (xs.shape[1], LANES))

    def prepare(part):
        wide = win[...].astype(jnp.float32)
        scales[part] = mods[part, 0].astype(jnp.float32)
        shifts = jnp.concatenate(
            [mods[part, 1], jnp.zeros((wide.shape[0] - per_dev, hidden), jnp.bfloat16)], axis=0)
        for pair in range(pairs):
            rows = []
            for at in (2 * pair, 2 * pair + 1):
                scaled = wide * jnp.broadcast_to(scales[part, at:at + 1, :], wide.shape)
                high = scaled.astype(jnp.bfloat16)
                low = (scaled - high.astype(jnp.float32)).astype(jnp.bfloat16)
                rows += [win[...], high, low, shifts]
            weights[part * pairs + pair] = jnp.concatenate(rows, axis=0).T

    def start_of(half):
        return xs[sample, :, half * LANES:(half + 1) * LANES]

    other = 1 - core
    found = {}
    total_of = {}

    def drift_at(sweep, half, index):
        key = (sweep, half, index)
        return found[key] if key in found else drifts[half, index]

    def sum_before(sweep, half, index, settled):
        key = (sweep, half, index)
        if index == 0:
            return None
        if sweep > 0 and settled and index <= sweep:
            return sum_before(sweep - 1, half, index, settled)
        if key not in total_of:
            before = sum_before(sweep, half, index - 1, settled)
            drift = drift_at(sweep, half, index - 1)
            total_of[key] = drift if before is None else before + drift
        return total_of[key]

    def opening(done):
        def task(part, pair, half, fresh, last):
            def right():
                if fresh:
                    if part is other:
                        for at, ref in enumerate((mods, steps)):
                            swap(at, ref, other).wait_recv()
                    prepare(part)
                return beside(column(start_of(half), 2 * pair), column(start_of(half), 2 * pair + 1))

            def finish(total):
                for at in range(2):
                    index = 2 * pair + at
                    drifts[half, part * per_dev + index] = (
                        total[:, at * LANES:(at + 1) * LANES] * step_of(index, part))
                if last:
                    done(half)

            return (part * pairs + pair, right, finish)

        return [
            task(part, pair, half, half == 0 and pair == 0, part is other and pair == pairs - 1)
            for part in (core, other) for half in range(2) for pair in range(pairs)
        ]

    def add(base, part):
        return base if part is None else base + part

    def whole(sweep, index, latent, done=None):
        def finish(total):
            for half in range(2):
                found[sweep, half, index] = total[:, half * LANES:(half + 1) * LANES] * step_of(index)
            if done is not None:
                done()

        return (
            index // 2, lambda: beside(*[column(latent(sweep - 1, half, index), index) for half in range(2)]), finish)

    def paired(sweep, pair, half, latent, done=None):
        def finish(total):
            for at in range(2):
                found[sweep, half, 2 * pair + at] = total[:, at * LANES:(at + 1) * LANES] * step_of(2 * pair + at)
            if done is not None:
                done()

        return (
            pair, lambda: beside(*[column(latent(sweep - 1, half, 2 * pair + at), 2 * pair + at) for at in range(2)]),
            finish)

    def base_copy(sweep, half):
        place = (sweep, slice(None), pl.ds(half * LANES, LANES))
        return pltpu.make_async_remote_copy(
            src_ref=base_out.at[place], dst_ref=base_in.at[place], send_sem=base_send.at[2 * sweep + half],
            recv_sem=base_recv.at[2 * sweep + half], device_id={"time": far}, device_id_type=MESH)

    def last_copy(at, source, half):
        lanes = pl.ds(half * LANES, LANES)
        return pltpu.make_async_remote_copy(
            src_ref=base_out.at[SWEEPS - 1, :, lanes], dst_ref=last_in.at[source, :, lanes],
            send_sem=last_send.at[2 * at + half], recv_sem=last_recv.at[2 * source + half],
            device_id={"time": (far, side)[at]}, device_id_type=MESH)

    def sums_copy(start, count):
        return pltpu.make_async_remote_copy(
            src_ref=sums.at[pl.ds(start, count)], dst_ref=sums_in.at[pl.ds(0, count)], send_sem=pair_send.at[2],
            recv_sem=pair_recv.at[2], device_id={"time": partner}, device_id_type=MESH)

    def hand_copy():
        return pltpu.make_async_remote_copy(
            src_ref=hand_out, dst_ref=hand_in, send_sem=pair_send.at[3],
            recv_sem=pair_recv.at[3], device_id={"time": partner}, device_id_type=MESH)

    def whole_sum(index, settled):
        values = [sum_before(SWEEPS - 1, half, index, settled) for half in range(2)]
        if values[0] is None:
            return jnp.zeros(xs.shape[1:], jnp.float32)
        return beside(*values)

    @pl.when(chip == 0)
    def _():
        found.clear(), total_of.clear()

        def latent(sweep, half, index):
            return add(start_of(half), sum_before(sweep, half, index, True))

        def put(sweep, half):
            base_out[sweep, :, half * LANES:(half + 1) * LANES] = latent(sweep, half, held)

        def send(sweep, half):
            put(sweep, half)
            if sweep == half == 0:
                pl.semaphore_wait(ready.at[1 - core], 1)
            base_copy(sweep, half).start()

        def send_last(half):
            put(SWEEPS - 1, half)
            if half == 0:
                pl.semaphore_wait(ready.at[core], 1)
            for at in (1, 0):
                last_copy(at, sample, half).start()

        tasks = opening(lambda half: send(0, half))
        for sweep in range(1, SWEEPS - 1):
            odd = sweep % 2 == 1
            for half in range(2):
                many = list(range((sweep + 1) // 2, held // 2))
                for pair in many:
                    close_now = pair == many[-1] and not (odd and half == 0)
                    tasks.append(paired(
                        sweep, pair, half, latent, functools.partial(send, sweep, half) if close_now else None))
                if odd and half == 0:
                    tasks.append(whole(sweep, sweep, latent, functools.partial(send, sweep, half)))
        tasks.append(whole(SWEEPS - 1, SWEEPS - 1, latent))
        for half in range(2):
            for pair in range(SWEEPS // 2, held // 2):
                tasks.append(paired(
                    SWEEPS - 1, pair, half, latent,
                    functools.partial(send_last, half) if pair == held // 2 - 1 else None))
        run(tasks)
        for index in range(held):
            sums[index] = whole_sum(index, True)
        sums_copy(other * per_dev, per_dev).start()
        out_ref[:, sample] = xs[sample] + sums[pl.ds(core * per_dev, per_dev)]
        sums_copy(0, per_dev).wait_recv()
        out_ref[:, 1 - sample] = xs[1 - sample] + sums_in[...]
        for sweep in range(SWEEPS - 1):
            for half in range(2):
                base_copy(sweep, half).wait_send()
        for at in range(2):
            for half in range(2):
                last_copy(at, sample, half).wait_send()
        sums_copy(0, per_dev).wait_send()

    def second_chip(which):
        found.clear(), total_of.clear()
        arrived = set()
        mine, theirs = (1 + which) % 2, which % 2
        last = SWEEPS - 1
        lent = {}

        def latent(sweep, half, index):
            if sweep < 0:
                return start_of(half)
            if (sweep, half) not in arrived:
                arrived.add((sweep, half))
                base_copy(sweep, half).wait_recv()
            base = base_in[sweep, :, half * LANES:(half + 1) * LANES]
            return add(base, sum_before(sweep, half, index, False))

        def hand():
            for half in range(2):
                hand_out[:, half * LANES:(half + 1) * LANES] = latent(last - 1, half, held - 2)
            hand_copy().start()

        def early():
            for index in range(per_dev):
                sums[index] = whole_sum(index, False)
            sums_copy(0, per_dev).start()

        def extra():
            def right():
                hand_copy().wait_recv()
                return beside(*[
                    column(hand_in[:, half * LANES:(half + 1) * LANES], held - 2) for half in range(2)])

            def finish(total):
                lent[0] = total * beside(step_of(held - 2), step_of(held - 2))

            return (held // 2 - 1, right, finish)

        for at, ref in enumerate((mods, steps)):
            swap(at, ref, other).wait_recv()
        prepare(0)
        prepare(1)
        tasks = []
        for sweep in range(SWEEPS):
            live = per_dev + sweep
            for half in range(2):
                for pair in range(live // 2):
                    done = None
                    if sweep == last and half == 1 and pair == 0 and which == 0:
                        done = hand
                    if sweep == last and half == 1 and pair == per_dev // 2 - 1 and which == 1:
                        done = early
                    tasks.append(paired(sweep, pair, half, latent, done))
            if live % 2 == 1 and not (sweep == last and which == 0):
                tasks.append(whole(sweep, live - 1, latent))
        if which == 1:
            tasks.append(extra())
        run(tasks)
        if which == 0:
            for index in range(per_dev, held - 1):
                sums[index] = whole_sum(index, False)
            sums_copy(per_dev, per_dev - 1).start()
        for source in range(2):
            for half in range(2):
                last_copy(0, source, half).wait_recv()
        for index in range(per_dev):
            out_ref[index, mine] = last_in[mine] + whole_sum(which * per_dev + index, False)
        if which == 0:
            sums_copy(0, per_dev).wait_recv()
            out_ref[:, theirs] = last_in[theirs] + sums_in[...]
            hand_copy().wait_send()
            sums_copy(0, per_dev - 1).wait_send()
        else:
            sums_copy(0, per_dev - 1).wait_recv()
            out_ref[:per_dev - 1, theirs] = last_in[theirs] + sums_in[:per_dev - 1]
            out_ref[per_dev - 1, theirs] = last_in[theirs] + (sums_in[per_dev - 2] + lent[0])
            sums_copy(0, per_dev).wait_send()

    for which in range(2):
        @pl.when(me == 2 + which)
        def _():
            second_chip(which)

    for at, ref in enumerate((mods, steps)):
        swap(at, ref, core).wait_send()


def solution(mesh):
    def local_run(x_init, w_in, w_out, mod_scale, mod_shift, step_size):
        samples, tokens, channels = x_init.shape
        per_dev, hidden = mod_scale.shape
        held = 2 * per_dev
        operands = (
            x_init.transpose(0, 2, 1), w_in, w_out.T, mod_scale, mod_shift, step_size.reshape(1, per_dev))
        latent = (channels, tokens)
        out = pl.pallas_call(
            kernel,
            out_shape=pltpu.VMEM((per_dev, samples) + latent, jnp.float32),
            in_specs=[pl.BlockSpec(memory_space=pl.ANY)] * len(operands),
            out_specs=pl.BlockSpec(memory_space=pltpu.VMEM),
            scratch_shapes=[
                pltpu.VMEM((samples,) + latent, jnp.float32),
                pltpu.VMEM((channels, hidden), jnp.bfloat16),
                pltpu.VMEM((channels, hidden), jnp.bfloat16),
                pltpu.VMEM((2, 2, per_dev, hidden), jnp.bfloat16),
                pltpu.VMEM((2, per_dev, hidden), jnp.float32),
                pltpu.VMEM((2, 1, per_dev), jnp.float32),
                pltpu.VMEM((per_dev, hidden, LANES), jnp.bfloat16),
                pltpu.VMEM((2, held, channels, LANES), jnp.float32),
                pltpu.VMEM((held,) + latent, jnp.float32),
                pltpu.VMEM((per_dev,) + latent, jnp.float32),
                pltpu.VMEM((SWEEPS,) + latent, jnp.float32),
                pltpu.VMEM((SWEEPS - 1,) + latent, jnp.float32),
                pltpu.VMEM((samples,) + latent, jnp.float32),
                pltpu.VMEM(latent, jnp.float32),
                pltpu.VMEM(latent, jnp.float32),
                pltpu.SemaphoreType.DMA((6,)),
                pltpu.SemaphoreType.DMA((4,)),
                pltpu.SemaphoreType.DMA((4,)),
                pltpu.SemaphoreType.DMA((2 * SWEEPS - 2,)),
                pltpu.SemaphoreType.DMA((2 * SWEEPS - 2,)),
                pltpu.SemaphoreType.DMA((4,)),
                pltpu.SemaphoreType.DMA((4,)),
                pltpu.SemaphoreType.REGULAR((2,)),
            ],
            compiler_params=pltpu.CompilerParams(
                collective_id=0, has_side_effects=True, vmem_limit_bytes=32 << 20),
        )(*[pltpu.with_memory_space_constraint(operand, pltpu.HBM) for operand in operands])
        return out.transpose(0, 1, 3, 2)

    return jax.shard_map(
        local_run,
        mesh=mesh,
        in_specs=(P(("part", "data"), None, None), P(None, None), P(None, None), P("time", None), P("time", None), P("time")),
        out_specs=P("time", ("part", "data"), None, None),
        check_vma=False,
    )
```

```python
import functools
import math

import jax
import jax.numpy as jnp
from jax import lax
from jax.experimental import pallas as pl
from jax.experimental.pallas import tpu as pltpu
from jax.sharding import PartitionSpec as P

SWEEPS = 4
ROWS = 256
LANES = 128
AHEAD = 3
BEHIND = 1
MESH = pl.DeviceIdType.MESH

A = 2.0 * math.sqrt(2.0 / math.pi)
B = 8.0 * math.sqrt(2.0 / math.pi) * 0.044715


def kernel(
    x_hbm, win_hbm, wout_hbm, scale_hbm, shift_hbm, step_hbm, out_ref,
    xs, win, wout, mods, scales, steps, weights, drifts, sums, sums_in, base_out, base_in, last_in, hand_out, hand_in,
    local_sem, pair_send, pair_recv, base_send, base_recv, last_send, last_recv, ready,
):
    me = lax.axis_index("time")
    chip, core = me // 2, lax.rem(me, 2)
    partner = 2 * chip + 1 - core
    far = 3 - me
    side = 2 * (1 - chip) + core
    sample = lax.rem(core + chip, 2)
    per_dev = mods.shape[2]
    hidden = win.shape[1]
    held = 2 * per_dev
    pairs = per_dev // 2

    loads = [
        pltpu.make_async_copy(source, target, local_sem.at[at])
        for at, (source, target) in enumerate((
            (scale_hbm, mods.at[core, 0]), (shift_hbm, mods.at[core, 1]), (step_hbm, steps.at[core]),
            (win_hbm, win), (x_hbm, xs), (wout_hbm, wout)))
    ]
    for load in loads:
        load.start()

    barrier = pltpu.get_barrier_semaphore()
    pl.semaphore_signal(barrier, inc=1, device_id={"time": partner}, device_id_type=MESH)

    @pl.when(chip == 0)
    def _():
        for peer in (far, side):
            pl.semaphore_signal(barrier, inc=1, device_id={"time": peer}, device_id_type=MESH)

    for load in loads[:3]:
        load.wait()
    pl.semaphore_wait(barrier, 1 + 2 * chip)

    def swap(at, ref, source):
        return pltpu.make_async_remote_copy(
            src_ref=ref.at[source], dst_ref=ref.at[source], send_sem=pair_send.at[at], recv_sem=pair_recv.at[at],
            device_id={"time": partner}, device_id_type=MESH)

    for at, ref in enumerate((mods, steps)):
        swap(at, ref, core).start()

    @pl.when(chip == 1)
    def _():
        for peer in (far, side):
            pl.semaphore_signal(ready.at[core], inc=1, device_id={"time": peer}, device_id_type=MESH)

    for load in loads[3:]:
        load.wait()

    def run(tasks):
        todo = [(task, slice(at, min(at + ROWS, hidden))) for task in tasks for at in range(0, hidden, ROWS)]
        halves, acts, right, total = {}, {}, {}, {}

        def first(step):
            task, at = todo[step]
            if at.start == 0:
                right[id(task)] = task[1]()
            halves[step] = jnp.dot(
                weights[task[0], at, :], right[id(task)], preferred_element_type=jnp.float32)

        def second(step):
            task, at = todo[step]
            part = jnp.dot(wout[:, at], acts.pop(step), preferred_element_type=jnp.float32)
            total[id(task)] = part if at.start == 0 else total[id(task)] + part
            if at.stop == hidden:
                task[2](total[id(task)])

        for step in range(min(AHEAD, len(todo))):
            first(step)
        for step in range(len(todo)):
            if step + AHEAD < len(todo):
                first(step + AHEAD)
            half = halves.pop(step)
            arg = half * (half * half * B + A)
            acts[step] = (half * jnp.tanh(arg) + half).astype(jnp.bfloat16)
            if step >= BEHIND:
                second(step - BEHIND)
        for step in range(max(len(todo) - BEHIND, 0), len(todo)):
            second(step)

    def column(latent, index):
        half = (latent * 0.5).astype(jnp.bfloat16)
        row = lax.broadcasted_iota(jnp.int32, half.shape, 0)
        unit = jnp.where(row == index % per_dev, 0.5, 0.0).astype(jnp.bfloat16)
        blank = [jnp.zeros_like(half)] * 4
        own = [half, half, half, unit]
        return jnp.concatenate(own + blank if index % 2 == 0 else blank + own, axis=0)

    def beside(left, right):
        return jnp.concatenate([left, right], axis=1)

    def step_of(index, part=None):
        part = index // per_dev if part is None else part
        at = index % per_dev
        return jnp.broadcast_to(steps[part][:, at:at + 1], (xs.shape[1], LANES))

    def prepare(part):
        wide = win[...].astype(jnp.float32)
        scales[part] = mods[part, 0].astype(jnp.float32)
        shifts = jnp.concatenate(
            [mods[part, 1], jnp.zeros((wide.shape[0] - per_dev, hidden), jnp.bfloat16)], axis=0)
        for pair in range(pairs):
            rows = []
            for at in (2 * pair, 2 * pair + 1):
                scaled = wide * jnp.broadcast_to(scales[part, at:at + 1, :], wide.shape)
                high = scaled.astype(jnp.bfloat16)
                low = (scaled - high.astype(jnp.float32)).astype(jnp.bfloat16)
                rows += [win[...], high, low, shifts]
            weights[part * pairs + pair] = jnp.concatenate(rows, axis=0).T

    def start_of(half):
        return xs[sample, :, half * LANES:(half + 1) * LANES]

    other = 1 - core
    found = {}
    total_of = {}

    def drift_at(sweep, half, index):
        key = (sweep, half, index)
        return found[key] if key in found else drifts[half, index]

    def sum_before(sweep, half, index, settled):
        key = (sweep, half, index)
        if index == 0:
            return None
        if sweep > 0 and settled and index <= sweep:
            return sum_before(sweep - 1, half, index, settled)
        if key not in total_of:
            before = sum_before(sweep, half, index - 1, settled)
            drift = drift_at(sweep, half, index - 1)
            total_of[key] = drift if before is None else before + drift
        return total_of[key]

    def opening(done):
        def task(part, pair, half, fresh, last):
            def right():
                if fresh:
                    if part is other:
                        for at, ref in enumerate((mods, steps)):
                            swap(at, ref, other).wait_recv()
                    prepare(part)
                return beside(column(start_of(half), 2 * pair), column(start_of(half), 2 * pair + 1))

            def finish(total):
                for at in range(2):
                    index = 2 * pair + at
                    drifts[half, part * per_dev + index] = (
                        total[:, at * LANES:(at + 1) * LANES] * step_of(index, part))
                if last:
                    done(half)

            return (part * pairs + pair, right, finish)

        return [
            task(part, pair, half, half == 0 and pair == 0, part is other and pair == pairs - 1)
            for part in (core, other) for half in range(2) for pair in range(pairs)
        ]

    def add(base, part):
        return base if part is None else base + part

    def whole(sweep, index, latent, done=None):
        def finish(total):
            for half in range(2):
                found[sweep, half, index] = total[:, half * LANES:(half + 1) * LANES] * step_of(index)
            if done is not None:
                done()

        return (
            index // 2, lambda: beside(*[column(latent(sweep - 1, half, index), index) for half in range(2)]), finish)

    def paired(sweep, pair, half, latent, done=None):
        def finish(total):
            for at in range(2):
                found[sweep, half, 2 * pair + at] = total[:, at * LANES:(at + 1) * LANES] * step_of(2 * pair + at)
            if done is not None:
                done()

        return (
            pair, lambda: beside(*[column(latent(sweep - 1, half, 2 * pair + at), 2 * pair + at) for at in range(2)]),
            finish)

    def base_copy(sweep, half):
        place = (sweep, slice(None), pl.ds(half * LANES, LANES))
        return pltpu.make_async_remote_copy(
            src_ref=base_out.at[place], dst_ref=base_in.at[place], send_sem=base_send.at[2 * sweep + half],
            recv_sem=base_recv.at[2 * sweep + half], device_id={"time": far}, device_id_type=MESH)

    def last_copy(at, source, half):
        lanes = pl.ds(half * LANES, LANES)
        return pltpu.make_async_remote_copy(
            src_ref=base_out.at[SWEEPS - 1, :, lanes], dst_ref=last_in.at[source, :, lanes],
            send_sem=last_send.at[2 * at + half], recv_sem=last_recv.at[2 * source + half],
            device_id={"time": (far, side)[at]}, device_id_type=MESH)

    def sums_copy(start, count):
        return pltpu.make_async_remote_copy(
            src_ref=sums.at[pl.ds(start, count)], dst_ref=sums_in.at[pl.ds(0, count)], send_sem=pair_send.at[2],
            recv_sem=pair_recv.at[2], device_id={"time": partner}, device_id_type=MESH)

    def hand_copy():
        return pltpu.make_async_remote_copy(
            src_ref=hand_out, dst_ref=hand_in, send_sem=pair_send.at[3],
            recv_sem=pair_recv.at[3], device_id={"time": partner}, device_id_type=MESH)

    def whole_sum(index, settled):
        values = [sum_before(SWEEPS - 1, half, index, settled) for half in range(2)]
        if values[0] is None:
            return jnp.zeros(xs.shape[1:], jnp.float32)
        return beside(*values)

    @pl.when(chip == 0)
    def _():
        found.clear(), total_of.clear()

        def latent(sweep, half, index):
            return add(start_of(half), sum_before(sweep, half, index, True))

        def put(sweep, half):
            base_out[sweep, :, half * LANES:(half + 1) * LANES] = latent(sweep, half, held)

        def send(sweep, half):
            put(sweep, half)
            if sweep == half == 0:
                for at in range(2):
                    pl.semaphore_wait(ready.at[at], 1)
            base_copy(sweep, half).start()

        def send_last(half):
            put(SWEEPS - 1, half)
            for at in (1, 0):
                last_copy(at, sample, half).start()

        tasks = opening(lambda half: send(0, half))
        for sweep in range(1, SWEEPS - 1):
            odd = sweep % 2 == 1
            for half in range(2):
                many = list(range((sweep + 1) // 2, held // 2))
                for pair in many:
                    close_now = pair == many[-1] and not (odd and half == 0)
                    tasks.append(paired(
                        sweep, pair, half, latent, functools.partial(send, sweep, half) if close_now else None))
                if odd and half == 0:
                    tasks.append(whole(sweep, sweep, latent, functools.partial(send, sweep, half)))
        tasks.append(whole(SWEEPS - 1, SWEEPS - 1, latent))
        for half in range(2):
            for pair in range(SWEEPS // 2, held // 2):
                tasks.append(paired(
                    SWEEPS - 1, pair, half, latent,
                    functools.partial(send_last, half) if pair == held // 2 - 1 else None))
        run(tasks)
        for index in range(held):
            sums[index] = whole_sum(index, True)
        sums_copy(other * per_dev, per_dev).start()
        out_ref[:, sample] = xs[sample] + sums[pl.ds(core * per_dev, per_dev)]
        sums_copy(0, per_dev).wait_recv()
        out_ref[:, 1 - sample] = xs[1 - sample] + sums_in[...]
        for sweep in range(SWEEPS - 1):
            for half in range(2):
                base_copy(sweep, half).wait_send()
        for at in range(2):
            for half in range(2):
                last_copy(at, sample, half).wait_send()
        sums_copy(0, per_dev).wait_send()

    def second_chip(which):
        found.clear(), total_of.clear()
        arrived = set()
        mine, theirs = (1 + which) % 2, which % 2
        last = SWEEPS - 1
        lent = {}

        def latent(sweep, half, index):
            if sweep < 0:
                return start_of(half)
            if (sweep, half) not in arrived:
                arrived.add((sweep, half))
                base_copy(sweep, half).wait_recv()
            base = base_in[sweep, :, half * LANES:(half + 1) * LANES]
            return add(base, sum_before(sweep, half, index, False))

        def hand():
            for half in range(2):
                hand_out[:, half * LANES:(half + 1) * LANES] = latent(last - 1, half, held - 2)
            hand_copy().start()

        def early():
            for index in range(per_dev):
                sums[index] = whole_sum(index, False)
            sums_copy(0, per_dev).start()

        def extra():
            def right():
                hand_copy().wait_recv()
                return beside(*[
                    column(hand_in[:, half * LANES:(half + 1) * LANES], held - 2) for half in range(2)])

            def finish(total):
                lent[0] = total * beside(step_of(held - 2), step_of(held - 2))

            return (held // 2 - 1, right, finish)

        for at, ref in enumerate((mods, steps)):
            swap(at, ref, other).wait_recv()
        prepare(0)
        prepare(1)
        tasks = []
        for sweep in range(SWEEPS):
            live = per_dev + sweep
            for half in range(2):
                for pair in range(live // 2):
                    done = None
                    if sweep == last and half == 1 and pair == 0 and which == 0:
                        done = hand
                    if sweep == last and half == 1 and pair == per_dev // 2 - 1 and which == 1:
                        done = early
                    tasks.append(paired(sweep, pair, half, latent, done))
            if live % 2 == 1 and not (sweep == last and which == 0):
                tasks.append(whole(sweep, live - 1, latent))
        if which == 1:
            tasks.append(extra())
        run(tasks)
        if which == 0:
            for index in range(per_dev, held - 1):
                sums[index] = whole_sum(index, False)
            sums_copy(per_dev, per_dev - 1).start()
        for source in range(2):
            for half in range(2):
                last_copy(0, source, half).wait_recv()
        for index in range(per_dev):
            out_ref[index, mine] = last_in[mine] + whole_sum(which * per_dev + index, False)
        if which == 0:
            sums_copy(0, per_dev).wait_recv()
            out_ref[:, theirs] = last_in[theirs] + sums_in[...]
            hand_copy().wait_send()
            sums_copy(0, per_dev - 1).wait_send()
        else:
            sums_copy(0, per_dev - 1).wait_recv()
            out_ref[:per_dev - 1, theirs] = last_in[theirs] + sums_in[:per_dev - 1]
            out_ref[per_dev - 1, theirs] = last_in[theirs] + (sums_in[per_dev - 2] + lent[0])
            sums_copy(0, per_dev).wait_send()

    for which in range(2):
        @pl.when(me == 2 + which)
        def _():
            second_chip(which)

    for at, ref in enumerate((mods, steps)):
        swap(at, ref, core).wait_send()


def solution(mesh):
    def local_run(x_init, w_in, w_out, mod_scale, mod_shift, step_size):
        samples, tokens, channels = x_init.shape
        per_dev, hidden = mod_scale.shape
        held = 2 * per_dev
        operands = (
            x_init.transpose(0, 2, 1), w_in, w_out.T, mod_scale, mod_shift, step_size.reshape(1, per_dev))
        latent = (channels, tokens)
        out = pl.pallas_call(
            kernel,
            out_shape=pltpu.VMEM((per_dev, samples) + latent, jnp.float32),
            in_specs=[pl.BlockSpec(memory_space=pl.ANY)] * len(operands),
            out_specs=pl.BlockSpec(memory_space=pltpu.VMEM),
            scratch_shapes=[
                pltpu.VMEM((samples,) + latent, jnp.float32),
                pltpu.VMEM((channels, hidden), jnp.bfloat16),
                pltpu.VMEM((channels, hidden), jnp.bfloat16),
                pltpu.VMEM((2, 2, per_dev, hidden), jnp.bfloat16),
                pltpu.VMEM((2, per_dev, hidden), jnp.float32),
                pltpu.VMEM((2, 1, per_dev), jnp.float32),
                pltpu.VMEM((per_dev, hidden, LANES), jnp.bfloat16),
                pltpu.VMEM((2, held, channels, LANES), jnp.float32),
                pltpu.VMEM((held,) + latent, jnp.float32),
                pltpu.VMEM((per_dev,) + latent, jnp.float32),
                pltpu.VMEM((SWEEPS,) + latent, jnp.float32),
                pltpu.VMEM((SWEEPS - 1,) + latent, jnp.float32),
                pltpu.VMEM((samples,) + latent, jnp.float32),
                pltpu.VMEM(latent, jnp.float32),
                pltpu.VMEM(latent, jnp.float32),
                pltpu.SemaphoreType.DMA((6,)),
                pltpu.SemaphoreType.DMA((4,)),
                pltpu.SemaphoreType.DMA((4,)),
                pltpu.SemaphoreType.DMA((2 * SWEEPS - 2,)),
                pltpu.SemaphoreType.DMA((2 * SWEEPS - 2,)),
                pltpu.SemaphoreType.DMA((4,)),
                pltpu.SemaphoreType.DMA((4,)),
                pltpu.SemaphoreType.REGULAR((2,)),
            ],
            compiler_params=pltpu.CompilerParams(
                collective_id=0, has_side_effects=True, vmem_limit_bytes=32 << 20),
        )(*[pltpu.with_memory_space_constraint(operand, pltpu.HBM) for operand in operands])
        return out.transpose(0, 1, 3, 2)

    return jax.shard_map(
        local_run,
        mesh=mesh,
        in_specs=(P(("part", "data"), None, None), P(None, None), P(None, None), P("time", None), P("time", None), P("time")),
        out_specs=P("time", ("part", "data"), None, None),
        check_vma=False,
    )
```

```python
import functools
import math

import jax
import jax.numpy as jnp
from jax import lax
from jax.experimental import pallas as pl
from jax.experimental.pallas import tpu as pltpu
from jax.sharding import PartitionSpec as P

SWEEPS = 4
ROWS = 256
LANES = 128
AHEAD = 3
BEHIND = 1
MESH = pl.DeviceIdType.MESH

A = 2.0 * math.sqrt(2.0 / math.pi)
B = 8.0 * math.sqrt(2.0 / math.pi) * 0.044715


def kernel(
    x_hbm, win_hbm, wout_hbm, scale_hbm, shift_hbm, step_hbm, out_ref,
    xs, win, wout, mods, scales, steps, weights, drifts, sums, sums_in, base_out, base_in, last_in, hand_out, hand_in,
    local_sem, pair_send, pair_recv, base_send, base_recv, last_send, last_recv, ready,
):
    me = lax.axis_index("time")
    chip, core = me // 2, lax.rem(me, 2)
    partner = 2 * chip + 1 - core
    far = 3 - me
    side = 2 * (1 - chip) + core
    sample = lax.rem(core + chip, 2)
    per_dev = mods.shape[2]
    hidden = win.shape[1]
    held = 2 * per_dev
    pairs = per_dev // 2

    loads = [
        pltpu.make_async_copy(source, target, local_sem.at[at])
        for at, (source, target) in enumerate((
            (scale_hbm, mods.at[core, 0]), (shift_hbm, mods.at[core, 1]), (step_hbm, steps.at[core]),
            (win_hbm, win), (x_hbm, xs), (wout_hbm, wout)))
    ]
    for load in loads:
        load.start()

    barrier = pltpu.get_barrier_semaphore()
    pl.semaphore_signal(barrier, inc=1, device_id={"time": partner}, device_id_type=MESH)

    @pl.when(chip == 0)
    def _():
        for peer in (far, side):
            pl.semaphore_signal(barrier, inc=1, device_id={"time": peer}, device_id_type=MESH)

    for load in loads[:3]:
        load.wait()
    pl.semaphore_wait(barrier, 1 + 2 * chip)

    def swap(at, ref, source):
        return pltpu.make_async_remote_copy(
            src_ref=ref.at[source], dst_ref=ref.at[source], send_sem=pair_send.at[at], recv_sem=pair_recv.at[at],
            device_id={"time": partner}, device_id_type=MESH)

    for at, ref in enumerate((mods, steps)):
        swap(at, ref, core).start()

    @pl.when(chip == 1)
    def _():
        for peer in (far, side):
            pl.semaphore_signal(ready.at[core], inc=1, device_id={"time": peer}, device_id_type=MESH)

    for load in loads[3:]:
        load.wait()

    def run(tasks):
        todo = [(task, slice(at, min(at + ROWS, hidden))) for task in tasks for at in range(0, hidden, ROWS)]
        halves, acts, right, total = {}, {}, {}, {}

        def first(step):
            task, at = todo[step]
            if at.start == 0:
                right[id(task)] = task[1]()
            halves[step] = jnp.dot(
                weights[task[0], at, :], right[id(task)], preferred_element_type=jnp.float32)

        def second(step):
            task, at = todo[step]
            part = jnp.dot(wout[:, at], acts.pop(step), preferred_element_type=jnp.float32)
            total[id(task)] = part if at.start == 0 else total[id(task)] + part
            if at.stop == hidden:
                task[2](total[id(task)])

        for step in range(min(AHEAD, len(todo))):
            first(step)
        for step in range(len(todo)):
            if step + AHEAD < len(todo):
                first(step + AHEAD)
            half = halves.pop(step)
            arg = half * (half * half * B + A)
            acts[step] = (half * jnp.tanh(arg) + half).astype(jnp.bfloat16)
            if step >= BEHIND:
                second(step - BEHIND)
        for step in range(max(len(todo) - BEHIND, 0), len(todo)):
            second(step)

    def column(latent, index):
        half = (latent * 0.5).astype(jnp.bfloat16)
        row = lax.broadcasted_iota(jnp.int32, half.shape, 0)
        unit = jnp.where(row == index % per_dev, 0.5, 0.0).astype(jnp.bfloat16)
        blank = [jnp.zeros_like(half)] * 4
        own = [half, half, half, unit]
        return jnp.concatenate(own + blank if index % 2 == 0 else blank + own, axis=0)

    def beside(left, right):
        return jnp.concatenate([left, right], axis=1)

    def step_of(index, part=None):
        part = index // per_dev if part is None else part
        at = index % per_dev
        return jnp.broadcast_to(steps[part][:, at:at + 1], (xs.shape[1], LANES))

    def prepare(part):
        wide = win[...].astype(jnp.float32)
        scales[part] = mods[part, 0].astype(jnp.float32)
        shifts = jnp.concatenate(
            [mods[part, 1], jnp.zeros((wide.shape[0] - per_dev, hidden), jnp.bfloat16)], axis=0)
        for pair in range(pairs):
            rows = []
            for at in (2 * pair, 2 * pair + 1):
                scaled = wide * jnp.broadcast_to(scales[part, at:at + 1, :], wide.shape)
                high = scaled.astype(jnp.bfloat16)
                low = (scaled - high.astype(jnp.float32)).astype(jnp.bfloat16)
                rows += [win[...], high, low, shifts]
            weights[part * pairs + pair] = jnp.concatenate(rows, axis=0).T

    def start_of(half):
        return xs[sample, :, half * LANES:(half + 1) * LANES]

    other = 1 - core
    found = {}
    total_of = {}

    def drift_at(sweep, half, index):
        key = (sweep, half, index)
        return found[key] if key in found else drifts[half, index]

    def sum_before(sweep, half, index, settled):
        key = (sweep, half, index)
        if index == 0:
            return None
        if sweep > 0 and settled and index <= sweep:
            return sum_before(sweep - 1, half, index, settled)
        if key not in total_of:
            before = sum_before(sweep, half, index - 1, settled)
            drift = drift_at(sweep, half, index - 1)
            total_of[key] = drift if before is None else before + drift
        return total_of[key]

    def opening(done):
        def task(part, pair, half, fresh, last):
            def right():
                if fresh:
                    if part is other:
                        for at, ref in enumerate((mods, steps)):
                            swap(at, ref, other).wait_recv()
                    prepare(part)
                return beside(column(start_of(half), 2 * pair), column(start_of(half), 2 * pair + 1))

            def finish(total):
                for at in range(2):
                    index = 2 * pair + at
                    drifts[half, part * per_dev + index] = (
                        total[:, at * LANES:(at + 1) * LANES] * step_of(index, part))
                if last:
                    done(half)

            return (part * pairs + pair, right, finish)

        return [
            task(part, pair, half, half == 0 and pair == 0, part is other and pair == pairs - 1)
            for part in (core, other) for half in range(2) for pair in range(pairs)
        ]

    def add(base, part):
        return base if part is None else base + part

    def whole(sweep, index, latent, done=None):
        def finish(total):
            for half in range(2):
                found[sweep, half, index] = total[:, half * LANES:(half + 1) * LANES] * step_of(index)
            if done is not None:
                done()

        return (
            index // 2, lambda: beside(*[column(latent(sweep - 1, half, index), index) for half in range(2)]), finish)

    def paired(sweep, pair, half, latent, done=None):
        def finish(total):
            for at in range(2):
                found[sweep, half, 2 * pair + at] = total[:, at * LANES:(at + 1) * LANES] * step_of(2 * pair + at)
            if done is not None:
                done()

        return (
            pair, lambda: beside(*[column(latent(sweep - 1, half, 2 * pair + at), 2 * pair + at) for at in range(2)]),
            finish)

    def base_copy(sweep, half):
        place = (sweep, slice(None), pl.ds(half * LANES, LANES))
        return pltpu.make_async_remote_copy(
            src_ref=base_out.at[place], dst_ref=base_in.at[place], send_sem=base_send.at[2 * sweep + half],
            recv_sem=base_recv.at[2 * sweep + half], device_id={"time": far}, device_id_type=MESH)

    def last_copy(at, source, half):
        lanes = pl.ds(half * LANES, LANES)
        return pltpu.make_async_remote_copy(
            src_ref=base_out.at[SWEEPS - 1, :, lanes], dst_ref=last_in.at[source, :, lanes],
            send_sem=last_send.at[2 * at + half], recv_sem=last_recv.at[2 * source + half],
            device_id={"time": (far, side)[at]}, device_id_type=MESH)

    def sums_copy(start, count):
        return pltpu.make_async_remote_copy(
            src_ref=sums.at[pl.ds(start, count)], dst_ref=sums_in.at[pl.ds(0, count)], send_sem=pair_send.at[2],
            recv_sem=pair_recv.at[2], device_id={"time": partner}, device_id_type=MESH)

    def hand_copy():
        return pltpu.make_async_remote_copy(
            src_ref=hand_out, dst_ref=hand_in, send_sem=pair_send.at[3],
            recv_sem=pair_recv.at[3], device_id={"time": partner}, device_id_type=MESH)

    def whole_sum(index, settled):
        values = [sum_before(SWEEPS - 1, half, index, settled) for half in range(2)]
        if values[0] is None:
            return jnp.zeros(xs.shape[1:], jnp.float32)
        return beside(*values)

    @pl.when(chip == 0)
    def _():
        found.clear(), total_of.clear()

        def latent(sweep, half, index):
            return add(start_of(half), sum_before(sweep, half, index, True))

        def put(sweep, half):
            base_out[sweep, :, half * LANES:(half + 1) * LANES] = latent(sweep, half, held)

        def send(sweep, half):
            put(sweep, half)
            if sweep == half == 0:
                for at in range(2):
                    pl.semaphore_wait(ready.at[at], 1)
            base_copy(sweep, half).start()

        def send_last(half):
            put(SWEEPS - 1, half)
            for at in (1, 0):
                last_copy(at, sample, half).start()

        tasks = opening(lambda half: send(0, half))
        for sweep in range(1, SWEEPS - 1):
            odd = sweep % 2 == 1
            for half in range(2):
                many = list(range((sweep + 1) // 2, held // 2))
                for pair in many:
                    close_now = pair == many[-1] and not (odd and half == 0)
                    tasks.append(paired(
                        sweep, pair, half, latent, functools.partial(send, sweep, half) if close_now else None))
                if odd and half == 0:
                    tasks.append(whole(sweep, sweep, latent, functools.partial(send, sweep, half)))
        tasks.append(whole(SWEEPS - 1, SWEEPS - 1, latent))
        for half in range(2):
            for pair in range(SWEEPS // 2, held // 2):
                tasks.append(paired(
                    SWEEPS - 1, pair, half, latent,
                    functools.partial(send_last, half) if pair == held // 2 - 1 else None))
        run(tasks)
        for index in range(held):
            sums[index] = whole_sum(index, True)
        sums_copy(other * per_dev, per_dev).start()
        out_ref[:, sample] = xs[sample] + sums[pl.ds(core * per_dev, per_dev)]
        sums_copy(0, per_dev).wait_recv()
        out_ref[:, 1 - sample] = xs[1 - sample] + sums_in[...]
        for sweep in range(SWEEPS - 1):
            for half in range(2):
                base_copy(sweep, half).wait_send()
        for at in range(2):
            for half in range(2):
                last_copy(at, sample, half).wait_send()
        sums_copy(0, per_dev).wait_send()

    def second_chip(which):
        found.clear(), total_of.clear()
        arrived = set()
        mine, theirs = (1 + which) % 2, which % 2
        last = SWEEPS - 1
        lent = {}

        def latent(sweep, half, index):
            if sweep < 0:
                return start_of(half)
            if (sweep, half) not in arrived:
                arrived.add((sweep, half))
                base_copy(sweep, half).wait_recv()
            base = base_in[sweep, :, half * LANES:(half + 1) * LANES]
            return add(base, sum_before(sweep, half, index, False))

        def hand():
            for half in range(2):
                hand_out[:, half * LANES:(half + 1) * LANES] = latent(last - 1, half, held - 2)
            hand_copy().start()

        def handed(right):
            value = right()
            hand()
            return value

        def early():
            for index in range(per_dev):
                sums[index] = whole_sum(index, False)
            sums_copy(0, per_dev).start()

        def extra():
            def right():
                hand_copy().wait_recv()
                return beside(*[
                    column(hand_in[:, half * LANES:(half + 1) * LANES], held - 2) for half in range(2)])

            def finish(total):
                lent[0] = total * beside(step_of(held - 2), step_of(held - 2))

            return (held // 2 - 1, right, finish)

        for at, ref in enumerate((mods, steps)):
            swap(at, ref, other).wait_recv()
        prepare(0)
        prepare(1)
        tasks = []
        for sweep in range(SWEEPS):
            live = per_dev + sweep
            for half in range(2):
                for pair in range(live // 2):
                    done = None
                    if sweep == last and half == 1 and pair == per_dev // 2 - 1 and which == 1:
                        done = early
                    task = paired(sweep, pair, half, latent, done)
                    if sweep == last and half == 1 and pair == 0 and which == 0:
                        task = (task[0], functools.partial(handed, task[1]), task[2])
                    tasks.append(task)
            if live % 2 == 1 and not (sweep == last and which == 0):
                tasks.append(whole(sweep, live - 1, latent))
        if which == 1:
            tasks.append(extra())
        run(tasks)
        if which == 0:
            for index in range(per_dev, held - 1):
                sums[index] = whole_sum(index, False)
            sums_copy(per_dev, per_dev - 1).start()
        for source in range(2):
            for half in range(2):
                last_copy(0, source, half).wait_recv()
        for index in range(per_dev):
            out_ref[index, mine] = last_in[mine] + whole_sum(which * per_dev + index, False)
        if which == 0:
            sums_copy(0, per_dev).wait_recv()
            out_ref[:, theirs] = last_in[theirs] + sums_in[...]
            hand_copy().wait_send()
            sums_copy(0, per_dev - 1).wait_send()
        else:
            sums_copy(0, per_dev - 1).wait_recv()
            out_ref[:per_dev - 1, theirs] = last_in[theirs] + sums_in[:per_dev - 1]
            out_ref[per_dev - 1, theirs] = last_in[theirs] + (sums_in[per_dev - 2] + lent[0])
            sums_copy(0, per_dev).wait_send()

    for which in range(2):
        @pl.when(me == 2 + which)
        def _():
            second_chip(which)

    for at, ref in enumerate((mods, steps)):
        swap(at, ref, core).wait_send()


def solution(mesh):
    def local_run(x_init, w_in, w_out, mod_scale, mod_shift, step_size):
        samples, tokens, channels = x_init.shape
        per_dev, hidden = mod_scale.shape
        held = 2 * per_dev
        operands = (
            x_init.transpose(0, 2, 1), w_in, w_out.T, mod_scale, mod_shift, step_size.reshape(1, per_dev))
        latent = (channels, tokens)
        out = pl.pallas_call(
            kernel,
            out_shape=pltpu.VMEM((per_dev, samples) + latent, jnp.float32),
            in_specs=[pl.BlockSpec(memory_space=pl.ANY)] * len(operands),
            out_specs=pl.BlockSpec(memory_space=pltpu.VMEM),
            scratch_shapes=[
                pltpu.VMEM((samples,) + latent, jnp.float32),
                pltpu.VMEM((channels, hidden), jnp.bfloat16),
                pltpu.VMEM((channels, hidden), jnp.bfloat16),
                pltpu.VMEM((2, 2, per_dev, hidden), jnp.bfloat16),
                pltpu.VMEM((2, per_dev, hidden), jnp.float32),
                pltpu.VMEM((2, 1, per_dev), jnp.float32),
                pltpu.VMEM((per_dev, hidden, LANES), jnp.bfloat16),
                pltpu.VMEM((2, held, channels, LANES), jnp.float32),
                pltpu.VMEM((held,) + latent, jnp.float32),
                pltpu.VMEM((per_dev,) + latent, jnp.float32),
                pltpu.VMEM((SWEEPS,) + latent, jnp.float32),
                pltpu.VMEM((SWEEPS - 1,) + latent, jnp.float32),
                pltpu.VMEM((samples,) + latent, jnp.float32),
                pltpu.VMEM(latent, jnp.float32),
                pltpu.VMEM(latent, jnp.float32),
                pltpu.SemaphoreType.DMA((6,)),
                pltpu.SemaphoreType.DMA((4,)),
                pltpu.SemaphoreType.DMA((4,)),
                pltpu.SemaphoreType.DMA((2 * SWEEPS - 2,)),
                pltpu.SemaphoreType.DMA((2 * SWEEPS - 2,)),
                pltpu.SemaphoreType.DMA((4,)),
                pltpu.SemaphoreType.DMA((4,)),
                pltpu.SemaphoreType.REGULAR((2,)),
            ],
            compiler_params=pltpu.CompilerParams(
                collective_id=0, has_side_effects=True, vmem_limit_bytes=32 << 20),
        )(*[pltpu.with_memory_space_constraint(operand, pltpu.HBM) for operand in operands])
        return out.transpose(0, 1, 3, 2)

    return jax.shard_map(
        local_run,
        mesh=mesh,
        in_specs=(P(("part", "data"), None, None), P(None, None), P(None, None), P("time", None), P("time", None), P("time")),
        out_specs=P("time", ("part", "data"), None, None),
        check_vma=False,
    )
```
